16 devices in a mesh: stage: 2 (over z), expert: 8 (over y, x, core).
Axes of the slice: x: 2, y: 2, z: 2, core: 2. Of those that a mesh axis runs over, the one named last changes fastest.
Arguments:
- x_act: bfloat16 [2, 16384, 1024], P('stage', 'expert')
- route_idx: int32 [2, 16384, 1], P('stage', 'expert')
- route_gate: float32 [2, 16384, 1], P('stage', 'expert')
- w_in1: bfloat16 [2, 128, 1024, 384], P('stage', 'expert')
- w_in3: bfloat16 [2, 128, 1024, 384], P('stage', 'expert')
- w_out: bfloat16 [2, 128, 384, 1024], P('stage', 'expert')
- ws_in1: bfloat16 [2, 1024, 384], P('stage')
- ws_in3: bfloat16 [2, 1024, 384], P('stage')
- ws_out: bfloat16 [2, 384, 1024], P('stage')
- dy_out: bfloat16 [2, 16384, 1024], P('stage', 'expert')
Outputs:
- output 1: bfloat16 [2, 16384, 1024], P('stage', 'expert')
- output 2: bfloat16 [2, 16384, 1024], P('stage', 'expert')
- output 3: bfloat16 [2, 128, 1024, 384], P('stage', 'expert')
- output 4: bfloat16 [2, 128, 1024, 384], P('stage', 'expert')
- output 5: bfloat16 [2, 128, 384, 1024], P('stage', 'expert')
- output 6: bfloat16 [2, 1024, 384], P('stage')
- output 7: bfloat16 [2, 1024, 384], P('stage')
- output 8: bfloat16 [2, 384, 1024], P('stage')
All inputs are finite; a program needn't handle non-finite values.
Results may differ from the reference program's by a relative error of at most 0.00662985.
Values are sent between devices in bfloat16 or wider.
A program may use at most 1 GiB of HBM per device.

```python
import jax
import jax.numpy as jnp
from jax import lax

STAGES = 2
EP_SIZE = 8
TOK_DEV = 2048
D_MODEL = 1024
FF_EXPERT = 384
SHARED_MULT = 1
EXPERTS = 128
TOP_K = 1
ROW_BLOCK = 32

LOCAL_EXP = EXPERTS // EP_SIZE
DEST_LIM = min(TOP_K, EP_SIZE)
MIN_DEST = (TOP_K + LOCAL_EXP - 1) // LOCAL_EXP
HOT_EXP = max(1, LOCAL_EXP // 4)
FF_SHARED = FF_EXPERT * SHARED_MULT
N_ROWS = EP_SIZE * TOK_DEV


def draw_routes(key):
    n_dev = STAGES * EP_SIZE
    key_perm, key_rot, key_size, key_coin, key_wide, key_hot = jax.random.split(key, 6)
    tok_perm = jax.vmap(lambda dev_key: jax.random.permutation(dev_key, TOK_DEV))(jax.random.split(key_perm, n_dev))
    residue = tok_perm % EP_SIZE
    rotate = jax.random.randint(key_rot, (n_dev, 1), 0, EP_SIZE)
    spread = jnp.where(residue < DEST_LIM, DEST_LIM, jax.random.randint(key_size, (n_dev, TOK_DEV), MIN_DEST, DEST_LIM + 1))
    base_dev = (residue + rotate) % EP_SIZE
    slot_ids = jnp.arange(TOP_K, dtype=jnp.int32)
    rel_dev = slot_ids % spread[:, :, None]
    slot_depth = slot_ids // spread[:, :, None]
    dest_dev = (base_dev[:, :, None] + rel_dev) % EP_SIZE
    shape3 = (n_dev, TOK_DEV, TOP_K)
    coin_flip = jax.random.randint(key_coin, shape3, 0, 2)
    start_all = jnp.where(coin_flip == 0, jax.random.randint(key_wide, shape3, 0, LOCAL_EXP), jax.random.randint(key_hot, shape3, 0, HOT_EXP))
    start_id = jnp.take_along_axis(start_all, rel_dev, axis=2)
    local_id = (start_id + slot_depth) % LOCAL_EXP
    return (dest_dev * LOCAL_EXP + local_id).astype(jnp.int32).reshape(STAGES, N_ROWS, TOP_K)


def setup_inputs(seed: int = 0) -> dict:
    keys = jax.random.split(jax.random.key(seed), 10)
    x_act = jax.random.normal(keys[0], (STAGES, N_ROWS, D_MODEL), jnp.float32).astype(jnp.bfloat16)
    route_idx = draw_routes(keys[1])
    route_gate = jax.random.uniform(keys[2], (STAGES, N_ROWS, TOP_K), jnp.float32, 0.5, 1.5) * TOP_K ** -0.5
    w_in1 = (jax.random.normal(keys[3], (STAGES, EXPERTS, D_MODEL, FF_EXPERT), jnp.float32) * D_MODEL ** -0.5).astype(jnp.bfloat16)
    w_in3 = (jax.random.normal(keys[4], (STAGES, EXPERTS, D_MODEL, FF_EXPERT), jnp.float32) * D_MODEL ** -0.5).astype(jnp.bfloat16)
    w_out = (jax.random.normal(keys[5], (STAGES, EXPERTS, FF_EXPERT, D_MODEL), jnp.float32) * FF_EXPERT ** -0.5).astype(jnp.bfloat16)
    ws_in1 = (jax.random.normal(keys[6], (STAGES, D_MODEL, FF_SHARED), jnp.float32) * D_MODEL ** -0.5).astype(jnp.bfloat16)
    ws_in3 = (jax.random.normal(keys[7], (STAGES, D_MODEL, FF_SHARED), jnp.float32) * D_MODEL ** -0.5).astype(jnp.bfloat16)
    ws_out = (jax.random.normal(keys[8], (STAGES, FF_SHARED, D_MODEL), jnp.float32) * FF_SHARED ** -0.5).astype(jnp.bfloat16)
    dy_out = jax.random.normal(keys[9], (STAGES, N_ROWS, D_MODEL), jnp.float32).astype(jnp.bfloat16)
    return dict(x_act=x_act, route_idx=route_idx, route_gate=route_gate, w_in1=w_in1, w_in3=w_in3, w_out=w_out, ws_in1=ws_in1, ws_in3=ws_in3, ws_out=ws_out, dy_out=dy_out)


def swiglu_grad(x_rows, go_rows, w_one, w_three, w_two):
    pre_a = jnp.dot(x_rows, w_one, preferred_element_type=jnp.float32)
    pre_b = jnp.dot(x_rows, w_three, preferred_element_type=jnp.float32)
    sig_a = jax.nn.sigmoid(pre_a)
    act_a = pre_a * sig_a
    hidden = (act_a * pre_b).astype(jnp.bfloat16)
    out_rows = jnp.dot(hidden, w_two, preferred_element_type=jnp.float32)
    grad_hid = jnp.dot(go_rows, w_two.T, preferred_element_type=jnp.float32)
    grad_a = (grad_hid * pre_b * sig_a * (1.0 + pre_a * (1.0 - sig_a))).astype(jnp.bfloat16)
    grad_b = (grad_hid * act_a).astype(jnp.bfloat16)
    dx_rows = jnp.dot(grad_a, w_one.T, preferred_element_type=jnp.float32) + jnp.dot(grad_b, w_three.T, preferred_element_type=jnp.float32)
    gw_one = jnp.dot(x_rows.T, grad_a, preferred_element_type=jnp.float32)
    gw_three = jnp.dot(x_rows.T, grad_b, preferred_element_type=jnp.float32)
    gw_two = jnp.dot(hidden.T, go_rows, preferred_element_type=jnp.float32)
    return out_rows, dx_rows, gw_one, gw_three, gw_two


def reference(x_act, route_idx, route_gate, w_in1, w_in3, w_out, ws_in1, ws_in3, ws_out, dy_out):
    n_groups = STAGES * EXPERTS
    n_pairs = STAGES * N_ROWS * TOP_K
    n_blocks = (n_pairs + ROW_BLOCK - 1) // ROW_BLOCK + n_groups
    x_recv = jnp.roll(x_act, 1, axis=0)
    x_flat = x_recv.reshape(STAGES * N_ROWS, D_MODEL)
    dy_flat = dy_out.reshape(STAGES * N_ROWS, D_MODEL)
    stage_off = (jnp.arange(STAGES, dtype=jnp.int32) * EXPERTS)[:, None, None]
    pair_key = (jnp.roll(route_idx, 1, axis=0) + stage_off).reshape(-1)
    pair_tok = jnp.arange(n_pairs, dtype=jnp.int32) // TOP_K
    pair_gate = jnp.roll(route_gate, 1, axis=0).reshape(-1)
    pair_order = jnp.argsort(pair_key, stable=True)
    sorted_key = pair_key[pair_order]
    counts = jnp.zeros((n_groups,), jnp.int32).at[pair_key].add(1)
    padded = (counts + ROW_BLOCK - 1) // ROW_BLOCK * ROW_BLOCK
    pad_end = jnp.cumsum(padded)
    pad_start = pad_end - padded
    cnt_start = jnp.cumsum(counts) - counts
    slot_pos = pad_start[sorted_key] + jnp.arange(n_pairs, dtype=jnp.int32) - cnt_start[sorted_key]
    slot_tok = jnp.zeros((n_blocks * ROW_BLOCK,), jnp.int32).at[slot_pos].set(pair_tok[pair_order])
    slot_gate = jnp.zeros((n_blocks * ROW_BLOCK,), jnp.float32).at[slot_pos].set(pair_gate[pair_order])
    block_key = jnp.minimum(jnp.searchsorted(pad_end, jnp.arange(n_blocks, dtype=jnp.int32) * ROW_BLOCK, side='right'), n_groups - 1)
    w1_flat = w_in1.reshape(n_groups, D_MODEL, FF_EXPERT)
    w3_flat = w_in3.reshape(n_groups, D_MODEL, FF_EXPERT)
    w2_flat = w_out.reshape(n_groups, FF_EXPERT, D_MODEL)

    def block_step(carry, block):
        y_acc, dx_acc, g_one, g_three, g_two = carry
        blk_key, blk_tok, blk_gate = block
        go_rows = (blk_gate[:, None] * dy_flat[blk_tok].astype(jnp.float32)).astype(jnp.bfloat16)
        out_rows, dx_rows, gw_one, gw_three, gw_two = swiglu_grad(x_flat[blk_tok], go_rows, w1_flat[blk_key], w3_flat[blk_key], w2_flat[blk_key])
        y_acc = y_acc.at[blk_tok].add(blk_gate[:, None] * out_rows)
        dx_acc = dx_acc.at[blk_tok].add(dx_rows)
        g_one = g_one.at[blk_key].add(gw_one)
        g_three = g_three.at[blk_key].add(gw_three)
        g_two = g_two.at[blk_key].add(gw_two)
        return (y_acc, dx_acc, g_one, g_three, g_two), None

    init = (jnp.zeros((STAGES * N_ROWS, D_MODEL), jnp.float32), jnp.zeros((STAGES * N_ROWS, D_MODEL), jnp.float32),
            jnp.zeros((n_groups, D_MODEL, FF_EXPERT), jnp.float32), jnp.zeros((n_groups, D_MODEL, FF_EXPERT), jnp.float32),
            jnp.zeros((n_groups, FF_EXPERT, D_MODEL), jnp.float32))
    final, _unused = lax.scan(block_step, init, (block_key, slot_tok.reshape(n_blocks, ROW_BLOCK), slot_gate.reshape(n_blocks, ROW_BLOCK)))
    y_acc, dx_acc, g_one, g_three, g_two = final

    def shared_stage(stage_args):
        xs_stage, dy_stage, u_one, u_three, u_two = stage_args
        return swiglu_grad(xs_stage, dy_stage, u_one, u_three, u_two)

    sh_out, sh_dx, gs_one, gs_three, gs_two = lax.map(shared_stage, (x_recv, dy_out, ws_in1, ws_in3, ws_out))
    y_out = (y_acc.reshape(STAGES, N_ROWS, D_MODEL) + sh_out).astype(jnp.bfloat16)
    dx_act = jnp.roll((dx_acc.reshape(STAGES, N_ROWS, D_MODEL) + sh_dx).astype(jnp.bfloat16), -1, axis=0)
    return (y_out, dx_act,
            g_one.reshape(STAGES, EXPERTS, D_MODEL, FF_EXPERT).astype(jnp.bfloat16),
            g_three.reshape(STAGES, EXPERTS, D_MODEL, FF_EXPERT).astype(jnp.bfloat16),
            g_two.reshape(STAGES, EXPERTS, FF_EXPERT, D_MODEL).astype(jnp.bfloat16),
            gs_one.astype(jnp.bfloat16), gs_three.astype(jnp.bfloat16), gs_two.astype(jnp.bfloat16))
```

```python
import functools

import jax
import jax.numpy as jnp
from jax import lax
from jax.experimental import pallas as pl
from jax.experimental.pallas import tpu as pltpu
from jax.sharding import PartitionSpec as P

BF16 = jnp.bfloat16
F32 = jnp.float32
MESH = pl.DeviceIdType.MESH
ALIGN = 16
TILE = 128
VMEM_BYTES = 66_000_000


def dot(lhs, rhs, lhs_dim=1, rhs_dim=0):
    return lax.dot_general(lhs, rhs, (((lhs_dim,), (rhs_dim,)), ((), ())), preferred_element_type=F32)


def onehot(values, axis_iota):
    return jnp.where(values == axis_iota, 1.0, 0.0).astype(BF16)


def flip(me, step):
    out = 0
    for weight in (4, 2, 1):
        mine = (me // weight) % 2
        mask = (step // weight) % 2
        out = out + weight * (mine + mask - 2 * mine * mask)
    return out


def greet_all(n_stage, n_group):
    stage, me = lax.axis_index('stage'), lax.axis_index('expert')
    barrier = pltpu.get_barrier_semaphore()
    for ds in range(n_stage):
        for dk in range(n_group):
            if ds or dk:
                pl.semaphore_signal(barrier, inc=1, device_id=((stage + ds) % n_stage, (me + dk) % n_group), device_id_type=MESH)
    pl.semaphore_wait(barrier, n_stage * n_group - 1)


def dispatch_kernel(n_local, n_rows, x_hbm, dy_hbm, ordx_ref, ordy_ref, meta_ref, xs_hbm, dys_hbm, gate_ref, pos_ref, bounds_ref,
                    x_v, dy_v, xp, dyp, xr, dyr, meta_r, xs, dys,
                    load_sem, xs_send, xs_recv, dy_send, dy_recv, m_send, m_recv, out_sem):
    stage, me = lax.axis_index('stage'), lax.axis_index('expert')
    n_group, cap = xr.shape[0], xr.shape[1]
    n_tok = x_v.shape[0]
    n_pos = n_rows - TILE
    load_x = pltpu.make_async_copy(x_hbm, x_v, load_sem.at[0])
    load_dy = pltpu.make_async_copy(dy_hbm, dy_v, load_sem.at[1])
    load_x.start()
    load_dy.start()
    greet_all(2, n_group)

    def meta_copy(step):
        peer = flip(me, step)
        return pltpu.make_async_remote_copy(src_ref=meta_ref.at[peer], dst_ref=meta_r.at[step], send_sem=m_send.at[step],
                                            recv_sem=m_recv.at[step], device_id=(1 - stage, peer), device_id_type=MESH)

    def x_copy(step):
        return pltpu.make_async_remote_copy(src_ref=xp.at[step], dst_ref=xr.at[step], send_sem=xs_send.at[step],
                                            recv_sem=xs_recv.at[step], device_id=(1 - stage, flip(me, step)), device_id_type=MESH)

    def dy_copy(step):
        return pltpu.make_async_remote_copy(src_ref=dyp.at[step], dst_ref=dyr.at[step], send_sem=dy_send.at[step],
                                            recv_sem=dy_recv.at[step], device_id=(stage, flip(me, step)), device_id_type=MESH)

    for step in range(n_group):
        meta_copy(step).start()
    load_x.wait()
    load_dy.wait()

    def send_step(step, carry):
        peer = flip(me, step)
        rows = pl.ds(pl.multiple_of(peer * cap, cap), cap)
        lanes = lax.broadcasted_iota(jnp.int32, (cap, n_tok), 1)
        xp[step] = dot(onehot(ordx_ref[rows, :], lanes), x_v[...]).astype(BF16)
        block = dot(onehot(ordy_ref[rows, :], lanes), dy_v[...]).astype(BF16)
        x_copy(step).start()

        @pl.when(step == 0)
        def _():
            dyr[0] = block

        @pl.when(step > 0)
        def _():
            dyp[step] = block
            dy_copy(step).start()
        return carry

    lax.fori_loop(0, n_group, send_step, 0)

    for ref in (xs, dys):
        ref[...] = jnp.zeros(ref.shape, BF16)
    gate_ref[...] = jnp.zeros(gate_ref.shape, F32)

    for step in range(n_group):
        meta_copy(step).wait()
    sub = lax.broadcasted_iota(jnp.int32, (n_local, cap), 0).astype(F32)
    hits = [jnp.where(meta_r[step, 0:1, :] == sub, 1.0, 0.0) for step in range(n_group)]
    counts = [jnp.sum(hit, axis=1, keepdims=True) for hit in hits]
    total = sum(counts[1:], counts[0])
    units = jnp.floor((total + (ALIGN - 1)) * (1.0 / ALIGN))
    lower = jnp.where(lax.broadcasted_iota(jnp.int32, (n_local, n_local), 1) < lax.broadcasted_iota(jnp.int32, (n_local, n_local), 0), 1.0, 0.0)
    first = dot(lower.astype(BF16), jnp.broadcast_to(units, (n_local, TILE)).astype(BF16)) * float(ALIGN)
    bounds_ref[0] = first.astype(jnp.int32)
    bounds_ref[1] = jnp.broadcast_to(total, (n_local, TILE)).astype(jnp.int32)
    earlier = jnp.where(lax.broadcasted_iota(jnp.int32, (cap, cap), 0) < lax.broadcasted_iota(jnp.int32, (cap, cap), 1), 1.0, 0.0).astype(BF16)
    base = first[:, 0:1]
    for step in range(n_group):
        rank = dot(hits[step].astype(BF16), earlier) + base
        pos_ref[step] = jnp.sum(hits[step] * rank, axis=0, keepdims=True).astype(jnp.int32)
        base = base + counts[step]

    def merge_step(step, carry):
        pos = pos_ref[step]
        gate = meta_r[step, 1:2, :]
        x_copy(step).wait()

        @pl.when(step > 0)
        def _():
            dy_copy(step).wait()

        def merge_rows(blk, inner):
            rows = pl.ds(pl.multiple_of(blk * cap, cap), cap)
            match = pos == lax.broadcasted_iota(jnp.int32, (cap, cap), 0) + blk * cap
            place = jnp.where(match, 1.0, 0.0).astype(BF16)
            xs[rows, :] += dot(place, xr[step]).astype(BF16)
            dys[rows, :] += dot(place, dyr[step]).astype(BF16)
            gate_ref[rows, :] += jnp.sum(jnp.where(match, gate, 0.0), axis=1, keepdims=True)
            return inner

        return lax.fori_loop(0, n_pos // cap, merge_rows, carry)

    lax.fori_loop(0, n_group, merge_step, 0)
    out_x = pltpu.make_async_copy(xs, xs_hbm, out_sem.at[0])
    out_dy = pltpu.make_async_copy(dys, dys_hbm, out_sem.at[1])
    out_x.start()
    out_dy.start()
    out_x.wait()
    out_dy.wait()


def dispatch(x_tok, dy_tok, ordx, ordy, meta, n_local, n_rows):
    n_group, cap = meta.shape[0], meta.shape[2]
    n_tok, width = x_tok.shape
    any_spec = pl.BlockSpec(memory_space=pl.ANY)
    vmem_spec = pl.BlockSpec(memory_space=pltpu.VMEM)
    dma = pltpu.SemaphoreType.DMA
    blocks = pltpu.VMEM((n_group, cap, width), BF16)
    return pl.pallas_call(
        functools.partial(dispatch_kernel, n_local, n_rows),
        out_shape=(jax.ShapeDtypeStruct((n_rows, width), BF16), jax.ShapeDtypeStruct((n_rows, width), BF16),
                   jax.ShapeDtypeStruct((n_rows, 1), F32), jax.ShapeDtypeStruct((n_group, 1, cap), jnp.int32),
                   jax.ShapeDtypeStruct((2, n_local, TILE), jnp.int32)),
        in_specs=[any_spec, any_spec, vmem_spec, vmem_spec, vmem_spec],
        out_specs=(any_spec, any_spec, vmem_spec, vmem_spec, vmem_spec),
        scratch_shapes=[pltpu.VMEM((n_tok, width), BF16), pltpu.VMEM((n_tok, width), BF16), blocks, blocks, blocks, blocks,
                        pltpu.VMEM(meta.shape, F32), pltpu.VMEM((n_rows, width), BF16), pltpu.VMEM((n_rows, width), BF16),
                        dma((2,)), dma((n_group,)), dma((n_group,)), dma((n_group,)), dma((n_group,)), dma((n_group,)), dma((n_group,)),
                        dma((2,))],
        compiler_params=pltpu.CompilerParams(collective_id=0, has_side_effects=True, vmem_limit_bytes=VMEM_BYTES),
        name='dispatch',
    )(x_tok, dy_tok, ordx, ordy, meta)


def swiglu_grads(pre_a, pre_b, grad_hid):
    sig_a = jax.nn.sigmoid(pre_a)
    act_a = pre_a * sig_a
    hidden = (act_a * pre_b).astype(BF16)
    grad_a = (grad_hid * pre_b * sig_a * (1.0 + pre_a * (1.0 - sig_a))).astype(BF16)
    grad_b = (grad_hid * act_a).astype(BF16)
    return hidden, grad_a, grad_b


def expert_kernel(first_ref, count_ref, xs_hbm, dys_hbm, gate_ref, w1, w3, w2, u1, u3, u2,
                  ys_hbm, dxs_hbm, g1, g3, g2, s1_hbm, s3_hbm, s2_hbm,
                  xs, dys, ys, dxs, hs, das, dbs, s1, s3, s2, acc1, acc3, acc2, sem, osem):
    expert = pl.program_id(0)
    n_rows = xs.shape[0]
    n_pos = n_rows - TILE

    @pl.when(expert == 0)
    def _():
        load_x = pltpu.make_async_copy(xs_hbm, xs, sem.at[0])
        load_dy = pltpu.make_async_copy(dys_hbm, dys, sem.at[1])
        load_x.start()
        load_dy.start()
        for ref in (ys, dxs):
            ref[...] = jnp.zeros(ref.shape, BF16)
        for ref in (s1, s3, s2):
            ref[...] = jnp.zeros(ref.shape, F32)
        for ref in (hs, das, dbs):
            ref[pl.ds(n_pos, TILE), :] = jnp.zeros((TILE, ref.shape[1]), BF16)
        load_x.wait()
        load_dy.wait()

        def shared_tile(blk, carry):
            rows = pl.ds(pl.multiple_of(blk * 2 * TILE, 2 * TILE), 2 * TILE)
            x_blk, dy_blk = xs[rows, :], dys[rows, :]
            hidden, grad_a, grad_b = swiglu_grads(dot(x_blk, u1[...]), dot(x_blk, u3[...]), dot(dy_blk, u2[...], 1, 1))
            hs[rows, :] = hidden
            das[rows, :] = grad_a
            dbs[rows, :] = grad_b
            s1[...] += dot(x_blk, grad_a, 0, 0)
            s3[...] += dot(x_blk, grad_b, 0, 0)
            s2[...] += dot(hidden, dy_blk, 0, 0)
            return carry

        lax.fori_loop(0, n_pos // (2 * TILE), shared_tile, 0)
        for k, (src, dst) in enumerate(((s1, s1_hbm), (s3, s3_hbm), (s2, s2_hbm))):
            pltpu.make_async_copy(src, dst, osem.at[k]).start()

    for ref in (acc1, acc3, acc2):
        ref[...] = jnp.zeros(ref.shape, F32)
    first, count = first_ref[expert], count_ref[expert]

    def tile_step(tile, carry):
        rows = pl.ds(pl.multiple_of(first + tile * TILE, ALIGN), TILE)
        x_blk, dy_blk, gate = xs[rows, :], dys[rows, :], gate_ref[rows, :]
        live = lax.broadcasted_iota(jnp.int32, (TILE, 1), 0) + tile * TILE < count
        grad_out = jnp.where(live, gate * dy_blk.astype(F32), 0.0).astype(BF16)
        hidden, grad_a, grad_b = swiglu_grads(dot(x_blk, w1[0]), dot(x_blk, w3[0]), dot(grad_out, w2[0], 1, 1))
        ys[rows, :] = (gate * dot(hidden, w2[0]) + dot(hs[rows, :], u2[...])).astype(BF16)
        dxs[rows, :] = ((dot(grad_a, w1[0], 1, 1) + dot(grad_b, w3[0], 1, 1))
                        + (dot(das[rows, :], u1[...], 1, 1) + dot(dbs[rows, :], u3[...], 1, 1))).astype(BF16)
        acc1[...] += dot(x_blk, grad_a, 0, 0)
        acc3[...] += dot(x_blk, grad_b, 0, 0)
        acc2[...] += dot(hidden, grad_out, 0, 0)
        return carry

    lax.fori_loop(0, (count + TILE - 1) // TILE, tile_step, 0)
    g1[0] = acc1[...].astype(BF16)
    g3[0] = acc3[...].astype(BF16)
    g2[0] = acc2[...].astype(BF16)

    @pl.when(expert == pl.num_programs(0) - 1)
    def _():
        out_y = pltpu.make_async_copy(ys, ys_hbm, sem.at[0])
        out_dx = pltpu.make_async_copy(dxs, dxs_hbm, sem.at[1])
        out_y.start()
        out_dx.start()
        for k, (src, dst) in enumerate(((s1, s1_hbm), (s3, s3_hbm), (s2, s2_hbm))):
            pltpu.make_async_copy(src, dst, osem.at[k]).wait()
        out_y.wait()
        out_dx.wait()


def experts(first, count, xs, dys, gate, w1, w3, w2, u1, u3, u2):
    n_rows, width = xs.shape
    n_local, _, ff = w1.shape
    fs = u1.shape[1]
    any_spec = pl.BlockSpec(memory_space=pl.ANY)
    one = dict(pipeline_mode=pl.Buffered(1))
    in_spec = pl.BlockSpec((1, width, ff), lambda e, *_: (e, 0, 0))
    out_spec = pl.BlockSpec((1, ff, width), lambda e, *_: (e, 0, 0))
    grid_spec = pltpu.PrefetchScalarGridSpec(
        num_scalar_prefetch=2, grid=(n_local,),
        in_specs=[any_spec, any_spec, pl.BlockSpec((n_rows, 1), lambda e, *_: (0, 0), **one), in_spec, in_spec, out_spec,
                  pl.BlockSpec((width, fs), lambda e, *_: (0, 0), **one), pl.BlockSpec((width, fs), lambda e, *_: (0, 0), **one),
                  pl.BlockSpec((fs, width), lambda e, *_: (0, 0), **one)],
        out_specs=(any_spec, any_spec, in_spec, in_spec, out_spec, any_spec, any_spec, any_spec),
        scratch_shapes=[pltpu.VMEM((n_rows, width), BF16) for _ in range(4)] + [pltpu.VMEM((n_rows, fs), BF16) for _ in range(3)]
        + [pltpu.VMEM((width, fs), F32), pltpu.VMEM((width, fs), F32), pltpu.VMEM((fs, width), F32)]
        + [pltpu.VMEM((width, ff), F32), pltpu.VMEM((width, ff), F32), pltpu.VMEM((ff, width), F32)]
        + [pltpu.SemaphoreType.DMA((2,)), pltpu.SemaphoreType.DMA((3,))])
    return pl.pallas_call(
        expert_kernel, grid_spec=grid_spec,
        out_shape=(jax.ShapeDtypeStruct((n_rows, width), BF16), jax.ShapeDtypeStruct((n_rows, width), BF16),
                   jax.ShapeDtypeStruct(w1.shape, BF16), jax.ShapeDtypeStruct(w3.shape, BF16), jax.ShapeDtypeStruct(w2.shape, BF16),
                   jax.ShapeDtypeStruct(u1.shape, F32), jax.ShapeDtypeStruct(u3.shape, F32), jax.ShapeDtypeStruct(u2.shape, F32)),
        compiler_params=pltpu.CompilerParams(vmem_limit_bytes=VMEM_BYTES, dimension_semantics=('arbitrary',)),
        name='experts',
    )(first, count, xs, dys, gate, w1, w3, w2, u1, u3, u2)


def return_kernel(ys_hbm, dxs_hbm, pos_ref, ordx_ref, ordy_ref, s1_ref, s3_ref, s2_ref, y_ref, dx_ref, f1, f3, f2,
                  ys, dxs, yp, dxp, yr, dxr, h1, h3, h2, r1, r3, r2, q1, q3, q2,
                  load_sem, y_send, y_recv, dx_send, dx_recv, half_send, half_recv, red_send, red_recv, all_send, all_recv, pair_send, pair_recv):
    stage, me = lax.axis_index('stage'), lax.axis_index('expert')
    n_group, cap = yr.shape[0], yr.shape[1]
    n_tok = y_ref.shape[0]
    n_pos = ys.shape[0]
    n_chip = n_group // 2
    chip, core = me // 2, me % 2
    load_y = pltpu.make_async_copy(ys_hbm.at[pl.ds(0, n_pos)], ys, load_sem.at[0])
    load_dx = pltpu.make_async_copy(dxs_hbm.at[pl.ds(0, n_pos)], dxs, load_sem.at[1])
    load_y.start()
    load_dx.start()
    greet_all(2, n_group)
    parts = ((s1_ref, h1, r1, q1, f1), (s3_ref, h3, r3, q3, f3), (s2_ref, h2, r2, q2, f2))

    def y_copy(step):
        return pltpu.make_async_remote_copy(src_ref=yp.at[step], dst_ref=yr.at[step], send_sem=y_send.at[step],
                                            recv_sem=y_recv.at[step], device_id=(stage, flip(me, step)), device_id_type=MESH)

    def dx_copy(step):
        return pltpu.make_async_remote_copy(src_ref=dxp.at[step], dst_ref=dxr.at[step], send_sem=dx_send.at[step],
                                            recv_sem=dx_recv.at[step], device_id=(1 - stage, flip(me, step)), device_id_type=MESH)

    def half_copy(k):
        src, dst = parts[k][0], parts[k][1]
        n = dst.shape[0]
        return pltpu.make_async_remote_copy(src_ref=src.at[pl.ds(pl.multiple_of((1 - core) * n, n), n)], dst_ref=dst, send_sem=half_send.at[k],
                                            recv_sem=half_recv.at[k], device_id=(stage, flip(me, 1)), device_id_type=MESH)

    def red_copy(k, hop):
        src, dst = parts[k][1], parts[k][2]
        n = dst.shape[1]
        there = flip(me, 2 * hop)
        return pltpu.make_async_remote_copy(src_ref=src.at[pl.ds(pl.multiple_of((there // 2) * n, n), n)], dst_ref=dst.at[hop - 1],
                                            send_sem=red_send.at[3 * k + hop - 1], recv_sem=red_recv.at[3 * k + hop - 1],
                                            device_id=(stage, there), device_id_type=MESH)

    def all_copy(k, hop, landing):
        own, full = parts[k][3], parts[k][4]
        n = own.shape[0]
        there = flip(me, 2 * hop)
        slot = (n_chip * core + (there // 2 if landing else chip)) * n
        return pltpu.make_async_remote_copy(src_ref=own, dst_ref=full.at[pl.ds(pl.multiple_of(slot, n), n)],
                                            send_sem=all_send.at[3 * k + hop - 1], recv_sem=all_recv.at[3 * k + hop - 1],
                                            device_id=(stage, there), device_id_type=MESH)

    def pair_copy(k, landing):
        full = parts[k][4]
        n = full.shape[0] // 2
        rows = pl.ds(pl.multiple_of(((1 - core) if landing else core) * n, n), n)
        return pltpu.make_async_remote_copy(src_ref=full.at[rows], dst_ref=full.at[rows], send_sem=pair_send.at[k],
                                            recv_sem=pair_recv.at[k], device_id=(stage, flip(me, 1)), device_id_type=MESH)

    for k in range(3):
        half_copy(k).start()
    load_y.wait()
    load_dx.wait()

    def send_step(step, carry):
        rows = pl.ds(pl.multiple_of(step * cap, cap), cap)
        pick = onehot(pos_ref[rows, :], lax.broadcasted_iota(jnp.int32, (cap, n_pos), 1))
        dxp[step] = dot(pick, dxs[...]).astype(BF16)
        block = dot(pick, ys[...]).astype(BF16)
        dx_copy(step).start()

        @pl.when(step == 0)
        def _():
            yr[0] = block
            for k in range(3):
                half_copy(k).wait()
            for src, half, _r, _q, _f in parts:
                n = half.shape[0]
                half[...] += src[pl.ds(pl.multiple_of(core * n, n), n), :]

        @pl.when(step > 0)
        def _():
            yp[step] = block
            y_copy(step).start()

        @pl.when(step == 1)
        def _():
            for k in range(3):
                for hop in (1, 2, 3):
                    red_copy(k, hop).start()
        return carry

    lax.fori_loop(0, n_group, send_step, 0)
    y_ref[...] = jnp.zeros(y_ref.shape, BF16)
    dx_ref[...] = jnp.zeros(dx_ref.shape, BF16)

    def home_step(step, carry):
        peer = flip(me, step)

        @pl.when(step > 0)
        def _():
            y_copy(step).wait()
        dx_copy(step).wait()
        ord_y, ord_x = ordy_ref[peer], ordx_ref[peer]

        def home_rows(blk, inner):
            rows = pl.ds(pl.multiple_of(blk * cap, cap), cap)
            tok = lax.broadcasted_iota(jnp.int32, (cap, cap), 0) + blk * cap
            y_ref[rows, :] += dot(onehot(ord_y, tok), yr[step]).astype(BF16)
            dx_ref[rows, :] += dot(onehot(ord_x, tok), dxr[step]).astype(BF16)
            return inner

        lax.fori_loop(0, n_tok // cap, home_rows, 0)

        @pl.when(step == 3)
        def _():
            for k in range(3):
                for hop in (1, 2, 3):
                    red_copy(k, hop).wait()
            for _s, half, recv, own, full in parts:
                n = own.shape[0]
                part = half[pl.ds(pl.multiple_of(chip * n, n), n), :] + recv[0] + recv[1] + recv[2]
                own[...] = part.astype(BF16)
                full[pl.ds(pl.multiple_of((n_chip * core + chip) * n, n), n), :] = part.astype(BF16)

        @pl.when(step == 4)
        def _():
            for k in range(3):
                for hop in (1, 2, 3):
                    all_copy(k, hop, False).start()

        @pl.when(step == 6)
        def _():
            for k in range(3):
                for hop in (1, 2, 3):
                    all_copy(k, hop, False).wait_send()
                    all_copy(k, hop, True).wait_recv()
            for k in range(3):
                pair_copy(k, False).start()
        return carry

    lax.fori_loop(0, n_group, home_step, 0)
    for k in range(3):
        pair_copy(k, False).wait_send()
        pair_copy(k, True).wait_recv()


def give_back(ys, dxs, pos, ordx, ordy, s1, s3, s2, n_tok):
    n_group, cap = ordx.shape[0], ordx.shape[2]
    n_rows, width = ys.shape
    n_pos = n_rows - TILE
    any_spec = pl.BlockSpec(memory_space=pl.ANY)
    vmem_spec = pl.BlockSpec(memory_space=pltpu.VMEM)
    dma = pltpu.SemaphoreType.DMA
    blocks = pltpu.VMEM((n_group, cap, width), BF16)
    grads = (s1, s3, s2)
    halves = [pltpu.VMEM((g.shape[0] // 2, g.shape[1]), F32) for g in grads]
    recvs = [pltpu.VMEM((3, g.shape[0] // n_group, g.shape[1]), F32) for g in grads]
    owns = [pltpu.VMEM((g.shape[0] // n_group, g.shape[1]), BF16) for g in grads]
    return pl.pallas_call(
        return_kernel,
        out_shape=(jax.ShapeDtypeStruct((n_tok, width), BF16), jax.ShapeDtypeStruct((n_tok, width), BF16),
                   *[jax.ShapeDtypeStruct(g.shape, BF16) for g in grads]),
        in_specs=[any_spec, any_spec] + [vmem_spec] * 6,
        out_specs=(vmem_spec,) * 5,
        scratch_shapes=[pltpu.VMEM((n_pos, width), BF16), pltpu.VMEM((n_pos, width), BF16), blocks, blocks, blocks, blocks]
        + halves + recvs + owns
        + [dma((2,)), dma((n_group,)), dma((n_group,)), dma((n_group,)), dma((n_group,)), dma((3,)), dma((3,)),
           dma((9,)), dma((9,)), dma((9,)), dma((9,)), dma((3,)), dma((3,))],
        compiler_params=pltpu.CompilerParams(collective_id=1, has_side_effects=True, vmem_limit_bytes=VMEM_BYTES),
        name='give_back',
    )(ys, dxs, pos, ordx, ordy, s1, s3, s2)


def solution(mesh):
    n_stage = mesh.shape['stage']
    n_group = mesh.shape['expert']
    fwd_perm = [(src, (src + 1) % n_stage) for src in range(n_stage)]
    tok_spec = P('stage', 'expert', None)
    w_spec = P('stage', 'expert', None, None)
    sh_spec = P('stage', None, None)

    def device_fn(x_act, route_idx, route_gate, w_in1, w_in3, w_out, ws_in1, ws_in3, ws_out, dy_out):
        n_tok = x_act.shape[1]
        n_local = w_in1.shape[1]
        cap = n_tok // n_group
        n_rows = n_tok + n_local * ALIGN + TILE
        idx = route_idx[0].reshape(n_tok)
        tok_ids = jnp.arange(n_tok, dtype=jnp.int32)
        sorted_idx, order, sorted_gate = lax.sort((idx, tok_ids, route_gate[0].reshape(n_tok)), num_keys=1)
        order_back = lax.ppermute(order, 'stage', fwd_perm)
        lid = (sorted_idx % n_local).astype(F32).reshape(n_group, 1, cap)
        meta = jnp.concatenate([lid, sorted_gate.reshape(n_group, 1, cap), jnp.zeros((n_group, 6, cap), F32)], axis=1)
        xs, dys, gate, pos, bounds = dispatch(x_act[0], dy_out[0], order[:, None], order_back[:, None], meta, n_local, n_rows)
        ys, dxs, g1, g3, g2, s1, s3, s2 = experts(bounds[0, :, 0], bounds[1, :, 0], xs, dys, gate,
                                                  w_in1[0], w_in3[0], w_out[0], ws_in1[0], ws_in3[0], ws_out[0])
        y_tok, dx_tok, f1, f3, f2 = give_back(ys, dxs, pos.reshape(n_tok, 1), order.reshape(n_group, 1, cap),
                                              order_back.reshape(n_group, 1, cap), s1, s3, s2, n_tok)
        return (y_tok[None], dx_tok[None], g1[None], g3[None], g2[None], f1[None], f3[None], f2[None])

    return jax.shard_map(device_fn, mesh=mesh,
                         in_specs=(tok_spec, tok_spec, tok_spec, w_spec, w_spec, w_spec, sh_spec, sh_spec, sh_spec, tok_spec),
                         out_specs=(tok_spec, tok_spec, w_spec, w_spec, w_spec, sh_spec, sh_spec, sh_spec),
                         check_vma=False)
```

```python
import functools

import jax
import jax.numpy as jnp
from jax import lax
from jax.experimental import pallas as pl
from jax.experimental.pallas import tpu as pltpu
from jax.sharding import PartitionSpec as P

BF16 = jnp.bfloat16
F32 = jnp.float32
MESH = pl.DeviceIdType.MESH
ALIGN = 16
TILE = 128
LAG = 2
PLACE = 2
VMEM_BYTES = 66_000_000


def dot(lhs, rhs, lhs_dim=1, rhs_dim=0):
    return lax.dot_general(lhs, rhs, (((lhs_dim,), (rhs_dim,)), ((), ())), preferred_element_type=F32)


def onehot(values, axis_iota):
    return jnp.where(values == axis_iota, 1.0, 0.0).astype(BF16)


def as_column(row):
    return jnp.broadcast_to(row, (TILE, row.shape[1])).T[:, 0:1]


def gate_parts(gate):
    high = gate.astype(BF16).astype(F32)
    middle = (gate - high).astype(BF16).astype(F32)
    low = gate - high - middle
    lane = lax.broadcasted_iota(jnp.int32, (gate.shape[0], TILE), 1)
    return jnp.where(lane == 0, high, jnp.where(lane == 1, middle, jnp.where(lane == 2, low, 0.0))).astype(BF16)


def flip(me, step):
    out = 0
    for weight in (4, 2, 1):
        mine = (me // weight) % 2
        mask = (step // weight) % 2
        out = out + weight * (mine + mask - 2 * mine * mask)
    return out


def stage_order(turn):
    pair, odd = turn // 2, turn % 2
    middle = ((pair + 1) // 2) % 2
    return middle * (1 + pair + 2 * odd) + (1 - middle) * (6 * (pair // 3) + odd)


def plane_order(turn):
    pair, odd = turn // 2, turn % 2
    opening = 1 - (pair + 1) // 2
    return opening * (6 + odd) + (1 - opening) * (3 + pair - 2 * odd)


def greet_all(n_stage, n_group):
    stage, me = lax.axis_index('stage'), lax.axis_index('expert')
    barrier = pltpu.get_barrier_semaphore()
    for ds in range(n_stage):
        for dk in range(n_group):
            if ds or dk:
                pl.semaphore_signal(barrier, inc=1, device_id=((stage + ds) % n_stage, (me + dk) % n_group), device_id_type=MESH)
    pl.semaphore_wait(barrier, n_stage * n_group - 1)


def swiglu_grads(pre, grad_hid):
    ff = grad_hid.shape[1]
    pre_a, pre_b = pre[:, :ff], pre[:, ff:]
    sig_a = jax.nn.sigmoid(pre_a)
    act_a = pre_a * sig_a
    hidden = (act_a * pre_b).astype(BF16)
    grad_a = (grad_hid * pre_b * sig_a * (1.0 + pre_a * (1.0 - sig_a))).astype(BF16)
    grad_b = (grad_hid * act_a).astype(BF16)
    return hidden, jnp.concatenate([grad_a, grad_b], axis=1)


def dispatch_kernel(n_local, n_rows, x_hbm, dy_hbm, ordx_ref, meta_ref, u1_hbm, u3_hbm, u2_hbm,
                    xs_hbm, dys_hbm, hdd_hbm, pos_ref, bounds_ref, ordz, p0, p1, p2, p3,
                    x_v, dy_v, xp, dyp, xr, dyr, meta_r, xs, dys, hdd, hddk, u13, u2, grads, half,
                    load_sem, xs_send, xs_recv, dy_send, dy_recv, m_send, m_recv, z_send, z_recv, h_send, h_recv, out_sem):
    stage, me = lax.axis_index('stage'), lax.axis_index('expert')
    chip, core = me // 2, me % 2
    n_group, cap = xr.shape[0], xr.shape[1]
    n_tok = x_v.shape[0]
    n_pos = n_rows - TILE
    ff = u2.shape[0]
    loads = [pltpu.make_async_copy(src, dst, load_sem.at[k]) for k, (src, dst) in enumerate((
        (x_hbm, x_v), (dy_hbm, dy_v), (u1_hbm, u13.at[:, pl.ds(0, ff)]), (u3_hbm, u13.at[:, pl.ds(ff, ff)]), (u2_hbm, u2)))]
    for load in loads:
        load.start()
    greet_all(2, n_group)

    def meta_copy(step):
        peer = flip(me, step)
        return pltpu.make_async_remote_copy(src_ref=meta_ref.at[peer], dst_ref=meta_r.at[step], send_sem=m_send.at[step],
                                            recv_sem=m_recv.at[step], device_id=(1 - stage, peer), device_id_type=MESH)

    def x_copy(step):
        return pltpu.make_async_remote_copy(src_ref=xp.at[step], dst_ref=xr.at[step], send_sem=xs_send.at[step],
                                            recv_sem=xs_recv.at[step], device_id=(1 - stage, flip(me, step)), device_id_type=MESH)

    def dy_copy(step):
        return pltpu.make_async_remote_copy(src_ref=dyp.at[step], dst_ref=dyr.at[step], send_sem=dy_send.at[step],
                                            recv_sem=dy_recv.at[step], device_id=(stage, flip(me, step)), device_id_type=MESH)

    def half_copy():
        n = half.shape[0]
        return pltpu.make_async_remote_copy(src_ref=grads.at[pl.ds(pl.multiple_of((1 - core) * n, n), n)], dst_ref=half, send_sem=h_send,
                                            recv_sem=h_recv, device_id=(stage, flip(me, 1)), device_id_type=MESH)

    def order_copy():
        return pltpu.make_async_remote_copy(src_ref=ordx_ref, dst_ref=ordz, send_sem=z_send, recv_sem=z_recv,
                                            device_id=(1 - stage, me), device_id_type=MESH)

    order_copy().start()
    for step in range(n_group):
        meta_copy(step).start()
    loads[0].wait()

    def permuted(order, src):
        return dot(onehot(as_column(order), lax.broadcasted_iota(jnp.int32, (cap, n_tok), 1)), src[...]).astype(BF16)

    def send_step(turn):
        step = stage_order(turn)
        xp[step] = permuted(ordx_ref[flip(me, step)], x_v)
        x_copy(step).start()

        @pl.when(turn == 0)
        def _():
            loads[1].wait()
            order_copy().wait()

        @pl.when(turn < 6)
        def _():
            plane = plane_order(turn)
            dyp[plane] = permuted(ordz[flip(me, plane)], dy_v)
            dy_copy(plane).start()

        @pl.when(turn < 2)
        def _():
            block = permuted(ordz[flip(me, turn)], dy_v)

            @pl.when(turn == 0)
            def _():
                dyr[0] = block

            @pl.when(turn == 1)
            def _():
                dyp[1] = block
                dy_copy(1).start()

    def place_rows(step, ref, block):
        pos = pos_ref[step]
        n = n_pos // PLACE

        def place_tile(blk, carry):
            rows = pl.ds(pl.multiple_of(blk * n, n), n)
            place = onehot(pos, lax.broadcasted_iota(jnp.int32, (n, cap), 0) + blk * n)
            ref[rows, :] += dot(place, block[...]).astype(BF16)
            return carry

        lax.fori_loop(0, PLACE, place_tile, 0)

    def shared_block(step):
        x_blk, dy_blk = xr[step], dyr[step]
        hidden, grad_ab = swiglu_grads(dot(x_blk, u13[...]), dot(dy_blk, u2[...], 1, 1))
        hddk[:, :ff] = hidden
        hddk[:, ff:3 * ff] = grad_ab
        hddk[:, 3 * ff:] = gate_parts(as_column(meta_r[step, 1:2, :]))
        grads[:, :2 * ff] += dot(x_blk, grad_ab, 0, 0)
        grads[:, 2 * ff:] += dot(dy_blk, hidden, 0, 0)
        place_rows(step, hdd, hddk)

    def merge_step(turn):
        @pl.when(turn < 6)
        def _():
            plane = plane_order(turn)
            dy_copy(plane).wait()
            place_rows(plane, dys, dyr.at[plane])

        @pl.when(turn < 2)
        def _():
            @pl.when(turn == 1)
            def _():
                dy_copy(1).wait()
            place_rows(turn, dys, dyr.at[turn])

        step = stage_order(turn)
        x_copy(step).wait()

        def shared_turn(back, carry):
            @pl.when(jnp.where(back == 0, (turn > 2) & (turn < 6), (turn < 2) | (turn > 4)))
            def _():
                shared_block(stage_order(turn - 1 + back))
            return carry

        lax.fori_loop(0, 2, shared_turn, 0)
        place_rows(step, xs, xr.at[step])

    def positions():
        for step in range(n_group):
            meta_copy(step).wait()
        sub = lax.broadcasted_iota(jnp.int32, (n_local, cap), 0).astype(F32)
        hits = [jnp.where(meta_r[step, 0:1, :] == sub, 1.0, 0.0) for step in range(n_group)]
        counts = [jnp.sum(hit, axis=1, keepdims=True) for hit in hits]
        total = sum(counts[1:], counts[0])
        units = jnp.floor((total + (ALIGN - 1)) * (1.0 / ALIGN))
        lower = jnp.where(lax.broadcasted_iota(jnp.int32, (n_local, n_local), 1) < lax.broadcasted_iota(jnp.int32, (n_local, n_local), 0), 1.0, 0.0)
        first = dot(lower.astype(BF16), jnp.broadcast_to(units, (n_local, TILE)).astype(BF16)) * float(ALIGN)
        bounds_ref[0] = first.astype(jnp.int32)
        bounds_ref[1] = jnp.broadcast_to(total, (n_local, TILE)).astype(jnp.int32)
        earlier = jnp.where(lax.broadcasted_iota(jnp.int32, (cap, cap), 0) < lax.broadcasted_iota(jnp.int32, (cap, cap), 1), 1.0, 0.0).astype(BF16)
        base = first[:, 0:1]
        for step in range(n_group):
            rank = dot(hits[step].astype(BF16), earlier) + base
            pos_ref[step] = jnp.sum(hits[step] * rank, axis=0, keepdims=True).astype(jnp.int32)
            base = base + counts[step]

    def both(step, carry):
        @pl.when(step < n_group)
        def _():
            send_step(step)

        @pl.when(step == 1)
        def _():
            for ref in (xs, dys, hdd):
                ref[...] = jnp.zeros(ref.shape, BF16)
            grads[...] = jnp.zeros(grads.shape, F32)
            positions()
            for load in loads[2:]:
                load.wait()

        @pl.when(step >= LAG)
        def _():
            merge_step(step - LAG)

        @pl.when(step == 5 + LAG)
        def _():
            outs[1].start()
        return carry

    outs = [pltpu.make_async_copy(src, dst, out_sem.at[k]) for k, (src, dst) in enumerate(((xs, xs_hbm), (dys, dys_hbm), (hdd, hdd_hbm)))]
    lax.fori_loop(0, n_group + LAG, both, 0)
    half_copy().start()
    outs[0].start()
    outs[2].start()
    half_copy().wait()
    n = p0.shape[0]
    for hop, ref in enumerate((p0, p1, p2, p3)):
        there = flip(me, 2 * hop) // 2
        ref[...] = grads[pl.ds(pl.multiple_of((4 * core + there) * n, n), n), :] + half[pl.ds(pl.multiple_of(there * n, n), n), :]
    for out in outs:
        out.wait()


def dispatch(x_tok, dy_tok, ordx, meta, u1, u3, u2, n_local, n_rows):
    n_group, cap = meta.shape[0], meta.shape[2]
    n_tok, width = x_tok.shape
    ff = u1.shape[1]
    any_spec = pl.BlockSpec(memory_space=pl.ANY)
    vmem_spec = pl.BlockSpec(memory_space=pltpu.VMEM)
    dma = pltpu.SemaphoreType.DMA
    blocks = pltpu.VMEM((n_group, cap, width), BF16)
    part = jax.ShapeDtypeStruct((width // n_group, 3 * ff), F32)
    return pl.pallas_call(
        functools.partial(dispatch_kernel, n_local, n_rows),
        out_shape=(jax.ShapeDtypeStruct((n_rows, width), BF16), jax.ShapeDtypeStruct((n_rows, width), BF16),
                   jax.ShapeDtypeStruct((n_rows, 3 * ff + TILE), BF16), jax.ShapeDtypeStruct((n_group, 1, cap), jnp.int32),
                   jax.ShapeDtypeStruct((2, n_local, TILE), jnp.int32),
                   jax.ShapeDtypeStruct(ordx.shape, jnp.int32), part, part, part, part),
        in_specs=[any_spec, any_spec, vmem_spec, vmem_spec, any_spec, any_spec, any_spec],
        out_specs=(any_spec, any_spec, any_spec) + (vmem_spec,) * 7,
        scratch_shapes=[pltpu.VMEM((n_tok, width), BF16), pltpu.VMEM((n_tok, width), BF16), blocks, blocks, blocks, blocks,
                        pltpu.VMEM(meta.shape, F32), pltpu.VMEM((n_rows, width), BF16), pltpu.VMEM((n_rows, width), BF16),
                        pltpu.VMEM((n_rows, 3 * ff + TILE), BF16), pltpu.VMEM((cap, 3 * ff + TILE), BF16),
                        pltpu.VMEM((width, 2 * ff), BF16), pltpu.VMEM((ff, width), BF16),
                        pltpu.VMEM((width, 3 * ff), F32), pltpu.VMEM((width // 2, 3 * ff), F32),
                        dma((5,)), dma((n_group,)), dma((n_group,)), dma((n_group,)), dma((n_group,)), dma((n_group,)), dma((n_group,)),
                        dma, dma, dma, dma, dma((3,))],
        compiler_params=pltpu.CompilerParams(collective_id=0, has_side_effects=True, vmem_limit_bytes=VMEM_BYTES),
        name='dispatch',
    )(x_tok, dy_tok, ordx, meta, u1, u3, u2)


N_IN = 3
N_CHUNK = 4


def expert_kernel(first_ref, count_ref, xs_hbm, dys_hbm, hdd_hbm, w1, w3, w2, u1_hbm, u3_hbm, u2_hbm,
                  ys_hbm, dxs_hbm, g1, g3, g2,
                  xs, dys, hdd, ys, dxs, u13, u2, w13_v, w2_v, o13, o2, acc13, acc2, sem, rsem, ssem, wsem, osem):
    n_local = w1.shape[0]
    ff = u2.shape[0]
    left, right = pl.ds(0, ff), pl.ds(ff, ff)
    chunk = xs.shape[0] // N_CHUNK
    loads = [pltpu.make_async_copy(src, dst, sem.at[k]) for k, (src, dst) in enumerate((
        (u1_hbm, u13.at[:, left]), (u3_hbm, u13.at[:, right]), (u2_hbm, u2)))]

    def row_loads(part):
        rows = pl.ds(pl.multiple_of(part * chunk, ALIGN), chunk)
        return [pltpu.make_async_copy(src.at[rows], dst.at[rows], rsem.at[part, k])
                for k, (src, dst) in enumerate(((xs_hbm, xs), (dys_hbm, dys), (hdd_hbm, hdd)))]

    def row_stores(part):
        rows = pl.ds(pl.multiple_of(part * chunk, ALIGN), chunk)
        return [pltpu.make_async_copy(src.at[rows], dst.at[rows], ssem.at[part, k]) for k, (src, dst) in enumerate(((ys, ys_hbm), (dxs, dxs_hbm)))]

    def weight_copies(expert):
        slot = lax.rem(expert, N_IN)
        return [pltpu.make_async_copy(w1.at[expert], w13_v.at[slot, :, left], wsem.at[slot, 0]),
                pltpu.make_async_copy(w3.at[expert], w13_v.at[slot, :, right], wsem.at[slot, 1]),
                pltpu.make_async_copy(w2.at[expert], w2_v.at[slot], wsem.at[slot, 2])]

    def grad_copies(expert):
        slot = lax.rem(expert, 2)
        return [pltpu.make_async_copy(o13.at[slot, :, left], g1.at[expert], osem.at[slot, 0]),
                pltpu.make_async_copy(o13.at[slot, :, right], g3.at[expert], osem.at[slot, 1]),
                pltpu.make_async_copy(o2.at[slot], g2.at[expert], osem.at[slot, 2])]

    for copy in row_loads(0) + weight_copies(0) + loads + weight_copies(1):
        copy.start()
    for part in range(1, N_CHUNK):
        for copy in row_loads(part):
            copy.start()
    for copy in weight_copies(2):
        copy.start()
    for ref in (ys, dxs):
        ref[...] = jnp.zeros(ref.shape, BF16)
    for load in loads:
        load.wait()

    def wait_rows(part, carry):
        for copy in row_loads(part):
            copy.wait()
        return carry

    def store_rows(part, carry):
        for copy in row_stores(part):
            copy.start()
        return carry

    def expert_step(expert, carry):
        loaded, stored = carry
        slot, oslot = lax.rem(expert, N_IN), lax.rem(expert, 2)
        for copy in weight_copies(expert):
            copy.wait()

        @pl.when(expert >= 2)
        def _():
            for copy in grad_copies(expert - 2):
                copy.wait()
        first, count = first_ref[expert], count_ref[expert]
        need = (first + jnp.maximum((count + TILE - 1) // TILE, 1) * TILE + chunk - 1) // chunk
        lax.fori_loop(loaded, need, wait_rows, 0)

        def rows_pass(begin, n):
            rows = pl.ds(pl.multiple_of(first + begin, ALIGN), n)
            x_blk, parts = xs[rows, :], hdd[rows, 3 * ff:].astype(F32)
            gate = parts[:, 0:1] + parts[:, 1:2] + parts[:, 2:3]
            live = lax.broadcasted_iota(jnp.int32, (n, 1), 0) + begin < count
            grad_out = jnp.where(live, gate * dys[rows, :].astype(F32), 0.0).astype(BF16)
            hidden, grad_ab = swiglu_grads(dot(x_blk, w13_v[slot]), dot(grad_out, w2_v[slot], 1, 1))
            ys[rows, :] = (gate * dot(hidden, w2_v[slot]) + dot(hdd[rows, :ff], u2[...])).astype(BF16)
            dxs[rows, :] = (dot(grad_ab, w13_v[slot], 1, 1) + dot(hdd[rows, ff:3 * ff], u13[...], 1, 1)).astype(BF16)
            return dot(x_blk, grad_ab, 0, 0), dot(hidden, grad_out, 0, 0)

        for n in (1, 2, 3):
            @pl.when((count > (n - 1) * TILE if n > 1 else count >= 0) & (count <= n * TILE))
            def _():
                grad13, grad2 = rows_pass(0, n * TILE)
                o13[oslot] = grad13.astype(BF16)
                o2[oslot] = grad2.astype(BF16)

        @pl.when(count > 3 * TILE)
        def _():
            acc13[...] = jnp.zeros(acc13.shape, F32)
            acc2[...] = jnp.zeros(acc2.shape, F32)

            def tile_step(tile, inner):
                grad13, grad2 = rows_pass(tile * TILE, TILE)
                acc13[...] += grad13
                acc2[...] += grad2
                return inner

            lax.fori_loop(0, (count + TILE - 1) // TILE, tile_step, 0)
            o13[oslot] = acc13[...].astype(BF16)
            o2[oslot] = acc2[...].astype(BF16)

        for copy in grad_copies(expert):
            copy.start()

        @pl.when(expert + N_IN < n_local)
        def _():
            for copy in weight_copies(expert + N_IN):
                copy.start()
        final = (first + (count + ALIGN - 1) // ALIGN * ALIGN) // chunk
        lax.fori_loop(stored, final, store_rows, 0)
        return jnp.maximum(loaded, need), jnp.maximum(stored, final)

    loaded, stored = lax.fori_loop(0, n_local, expert_step, (0, 0))
    lax.fori_loop(loaded, N_CHUNK, wait_rows, 0)
    lax.fori_loop(stored, N_CHUNK, store_rows, 0)
    for copy in grad_copies(n_local - 2) + grad_copies(n_local - 1):
        copy.wait()
    for part in range(N_CHUNK):
        for copy in row_stores(part):
            copy.wait()


def experts(first, count, xs, dys, hdd, w1, w3, w2, u1, u3, u2):
    n_rows, width = xs.shape
    ff = w1.shape[2]
    any_spec = pl.BlockSpec(memory_space=pl.ANY)
    smem_spec = pl.BlockSpec(memory_space=pltpu.SMEM)
    rows = pltpu.VMEM((n_rows, width), BF16)
    return pl.pallas_call(
        expert_kernel,
        in_specs=[smem_spec, smem_spec, any_spec, any_spec, any_spec] + [any_spec] * 6,
        out_specs=(any_spec,) * 5,
        out_shape=(jax.ShapeDtypeStruct((n_rows, width), BF16), jax.ShapeDtypeStruct((n_rows, width), BF16),
                   jax.ShapeDtypeStruct(w1.shape, BF16), jax.ShapeDtypeStruct(w3.shape, BF16), jax.ShapeDtypeStruct(w2.shape, BF16)),
        scratch_shapes=[rows, rows, pltpu.VMEM(hdd.shape, BF16), rows, rows,
                        pltpu.VMEM((width, 2 * ff), BF16), pltpu.VMEM((ff, width), BF16),
                        pltpu.VMEM((N_IN, width, 2 * ff), BF16), pltpu.VMEM((N_IN, ff, width), BF16),
                        pltpu.VMEM((2, width, 2 * ff), BF16), pltpu.VMEM((2, ff, width), BF16),
                        pltpu.VMEM((width, 2 * ff), F32), pltpu.VMEM((ff, width), F32),
                        pltpu.SemaphoreType.DMA((3,)), pltpu.SemaphoreType.DMA((N_CHUNK, 3)), pltpu.SemaphoreType.DMA((N_CHUNK, 2)),
                        pltpu.SemaphoreType.DMA((N_IN, 3)), pltpu.SemaphoreType.DMA((2, 3))],
        compiler_params=pltpu.CompilerParams(vmem_limit_bytes=VMEM_BYTES),
        cost_estimate=pl.CostEstimate(flops=40_000_000_000, bytes_accessed=100_000_000, transcendentals=0),
        name='experts',
    )(first, count, xs, dys, hdd, w1, w3, w2, u1, u3, u2)


def return_kernel(ys_hbm, dxs_hbm, pos_ref, ordx_ref, ordy_ref, p0, r1, r2, r3, y_ref, dx_ref, f1, f3, f2,
                  ys, dxs, yp, dxp, yr, dxr, own, own2, all13, all2,
                  load_sem, y_send, y_recv, dx_send, dx_recv, all_send, all_recv, pair_send, pair_recv):
    stage, me = lax.axis_index('stage'), lax.axis_index('expert')
    n_group, cap = yr.shape[0], yr.shape[1]
    n_tok = y_ref.shape[0]
    n_pos = ys.shape[0]
    n_chip = n_group // 2
    chip, core = me // 2, me % 2
    ff = f1.shape[1]
    n_part = own.shape[0]
    load_y = pltpu.make_async_copy(ys_hbm.at[pl.ds(0, n_pos)], ys, load_sem.at[0])
    load_dx = pltpu.make_async_copy(dxs_hbm.at[pl.ds(0, n_pos)], dxs, load_sem.at[1])
    load_dx.start()
    load_y.start()
    greet_all(2, n_group)

    def y_copy(step):
        return pltpu.make_async_remote_copy(src_ref=yp.at[step], dst_ref=yr.at[step], send_sem=y_send.at[step],
                                            recv_sem=y_recv.at[step], device_id=(stage, flip(me, step)), device_id_type=MESH)

    def dx_copy(step):
        return pltpu.make_async_remote_copy(src_ref=dxp.at[step], dst_ref=dxr.at[step], send_sem=dx_send.at[step],
                                            recv_sem=dx_recv.at[step], device_id=(1 - stage, flip(me, step)), device_id_type=MESH)

    def all_copies(hop, landing):
        there = flip(me, 2 * hop)
        slot = n_chip * core + (there // 2 if landing else chip)
        return [pltpu.make_async_remote_copy(src_ref=src, dst_ref=dst.at[slot], send_sem=all_send.at[2 * hop - 2 + k],
                                             recv_sem=all_recv.at[2 * hop - 2 + k], device_id=(stage, there), device_id_type=MESH)
                for k, (src, dst) in enumerate(((own, all13), (own2, all2)))]

    def pair_copies(landing):
        rows = pl.ds(((1 - core) if landing else core) * n_chip, n_chip)
        return [pltpu.make_async_remote_copy(src_ref=ref.at[rows], dst_ref=ref.at[rows], send_sem=pair_send.at[k],
                                             recv_sem=pair_recv.at[k], device_id=(stage, flip(me, 1)), device_id_type=MESH)
                for k, ref in enumerate((all13, all2))]

    part = p0[...] + r1[...] + r2[...] + r3[...]
    own[...] = part[:, :2 * ff].astype(BF16)
    own2[...] = part[:, 2 * ff:].T.astype(BF16)
    all13[n_chip * core + chip] = part[:, :2 * ff].astype(BF16)
    all2[n_chip * core + chip] = part[:, 2 * ff:].T.astype(BF16)
    load_dx.wait()

    def picked(step, src):
        return dot(onehot(as_column(pos_ref[step]), lax.broadcasted_iota(jnp.int32, (cap, n_pos), 1)), src[...]).astype(BF16)

    def send_step(turn):
        step = stage_order(turn)
        dxp[step] = picked(step, dxs)
        dx_copy(step).start()

        @pl.when(turn == 0)
        def _():
            load_y.wait()

        @pl.when(turn < 6)
        def _():
            plane = plane_order(turn)
            yp[plane] = picked(plane, ys)
            y_copy(plane).start()

        @pl.when(turn < 2)
        def _():
            block = picked(turn, ys)

            @pl.when(turn == 0)
            def _():
                yr[0] = block

            @pl.when(turn == 1)
            def _():
                yp[1] = block
                y_copy(1).start()

    def home_rows(order, ref, block):
        n = n_tok // PLACE

        def home_tile(blk, carry):
            rows = pl.ds(pl.multiple_of(blk * n, n), n)
            tok = lax.broadcasted_iota(jnp.int32, (n, cap), 0) + blk * n
            ref[rows, :] += dot(onehot(order, tok), block[...]).astype(BF16)
            return carry

        lax.fori_loop(0, PLACE, home_tile, 0)

    def home_step(turn):
        @pl.when(turn < 6)
        def _():
            plane = plane_order(turn)
            y_copy(plane).wait()
            home_rows(ordy_ref[flip(me, plane)], y_ref, yr.at[plane])

        @pl.when(turn < 2)
        def _():
            @pl.when(turn == 1)
            def _():
                y_copy(1).wait()
            home_rows(ordy_ref[flip(me, turn)], y_ref, yr.at[turn])

        step = stage_order(turn)
        dx_copy(step).wait()
        home_rows(ordx_ref[flip(me, step)], dx_ref, dxr.at[step])

    def both(step, carry):
        @pl.when(step < n_group)
        def _():
            send_step(step)

        @pl.when(step == 1)
        def _():
            y_ref[...] = jnp.zeros(y_ref.shape, BF16)
            dx_ref[...] = jnp.zeros(dx_ref.shape, BF16)
            for hop in (1, 2, 3):
                for copy in all_copies(hop, False):
                    copy.start()

        @pl.when(step >= LAG)
        def _():
            home_step(step - LAG)

        @pl.when(step == 6)
        def _():
            for hop in (1, 2, 3):
                for copy in all_copies(hop, False):
                    copy.wait_send()
                for copy in all_copies(hop, True):
                    copy.wait_recv()
            for copy in pair_copies(False):
                copy.start()

        @pl.when(step == 8)
        def _():
            for copy in pair_copies(False):
                copy.wait_send()
            for copy in pair_copies(True):
                copy.wait_recv()
            for k in range(n_group):
                rows = pl.ds(k * n_part, n_part)
                f1[rows, :] = all13[k, :, :ff]
                f3[rows, :] = all13[k, :, ff:]
                f2[:, rows] = all2[k]
        return carry

    lax.fori_loop(0, n_group + LAG, both, 0)


def give_back(ys, dxs, pos, ordx, ordy, p0, r1, r2, r3, n_tok):
    n_group, cap = ordx.shape[0], ordx.shape[2]
    n_rows, width = ys.shape
    n_pos = n_rows - TILE
    n_part, ff = p0.shape[0], p0.shape[1] // 3
    any_spec = pl.BlockSpec(memory_space=pl.ANY)
    vmem_spec = pl.BlockSpec(memory_space=pltpu.VMEM)
    dma = pltpu.SemaphoreType.DMA
    blocks = pltpu.VMEM((n_group, cap, width), BF16)
    in_shape = jax.ShapeDtypeStruct((width, ff), BF16)
    return pl.pallas_call(
        return_kernel,
        out_shape=(jax.ShapeDtypeStruct((n_tok, width), BF16), jax.ShapeDtypeStruct((n_tok, width), BF16),
                   in_shape, in_shape, jax.ShapeDtypeStruct((ff, width), BF16)),
        in_specs=[any_spec, any_spec] + [vmem_spec] * 7,
        out_specs=(vmem_spec,) * 5,
        scratch_shapes=[pltpu.VMEM((n_pos, width), BF16), pltpu.VMEM((n_pos, width), BF16), blocks, blocks, blocks, blocks,
                        pltpu.VMEM((n_part, 2 * ff), BF16), pltpu.VMEM((ff, n_part), BF16),
                        pltpu.VMEM((n_group, n_part, 2 * ff), BF16), pltpu.VMEM((n_group, ff, n_part), BF16),
                        dma((2,)), dma((n_group,)), dma((n_group,)), dma((n_group,)), dma((n_group,)),
                        dma((6,)), dma((6,)), dma((2,)), dma((2,))],
        compiler_params=pltpu.CompilerParams(collective_id=1, has_side_effects=True, vmem_limit_bytes=VMEM_BYTES),
        name='give_back',
    )(ys, dxs, pos, ordx, ordy, p0, r1, r2, r3)


def solution(mesh):
    n_group = mesh.shape['expert']
    tok_spec = P('stage', 'expert', None)
    w_spec = P('stage', 'expert', None, None)
    sh_spec = P('stage', None, None)

    def device_fn(x_act, route_idx, route_gate, w_in1, w_in3, w_out, ws_in1, ws_in3, ws_out, dy_out):
        n_tok = x_act.shape[1]
        n_local = w_in1.shape[1]
        cap = n_tok // n_group
        n_rows = n_tok + n_local * ALIGN + TILE
        idx = route_idx[0].reshape(n_tok)
        tok_ids = jnp.arange(n_tok, dtype=jnp.int32)
        sorted_idx, order, sorted_gate = lax.sort((idx, tok_ids, route_gate[0].reshape(n_tok)), num_keys=1)
        order = order.reshape(n_group, 1, cap)
        lid = (sorted_idx % n_local).astype(F32).reshape(n_group, 1, cap)
        meta = jnp.concatenate([lid, sorted_gate.reshape(n_group, 1, cap), jnp.zeros((n_group, 6, cap), F32)], axis=1)
        xs, dys, hdd, pos, bounds, order_back, p0, p1, p2, p3 = dispatch(
            x_act[0], dy_out[0], order, meta, ws_in1[0], ws_in3[0], ws_out[0], n_local, n_rows)
        recv = [lax.ppermute(part, 'expert', [(k, k ^ (2 * hop)) for k in range(n_group)]) for hop, part in ((1, p1), (2, p2), (3, p3))]
        ys, dxs, g1, g3, g2 = experts(bounds[0, :, 0], bounds[1, :, 0], xs, dys, hdd,
                                      w_in1[0], w_in3[0], w_out[0], ws_in1[0], ws_in3[0], ws_out[0])
        y_tok, dx_tok, f1, f3, f2 = give_back(ys, dxs, pos, order, order_back, p0, *recv, n_tok)
        return (y_tok[None], dx_tok[None], g1[None], g3[None], g2[None], f1[None], f3[None], f2[None])

    return jax.shard_map(device_fn, mesh=mesh,
                         in_specs=(tok_spec, tok_spec, tok_spec, w_spec, w_spec, w_spec, sh_spec, sh_spec, sh_spec, tok_spec),
                         out_specs=(tok_spec, tok_spec, w_spec, w_spec, w_spec, sh_spec, sh_spec, sh_spec),
                         check_vma=False)
```

```python
import functools

import jax
import jax.numpy as jnp
from jax import lax
from jax.experimental import pallas as pl
from jax.experimental.pallas import tpu as pltpu
from jax.sharding import PartitionSpec as P

BF16 = jnp.bfloat16
F32 = jnp.float32
MESH = pl.DeviceIdType.MESH
ALIGN = 16
TILE = 128
AHEAD = 2
PLACE = 2
VMEM_BYTES = 66_000_000


def dot(lhs, rhs, lhs_dim=1, rhs_dim=0):
    return lax.dot_general(lhs, rhs, (((lhs_dim,), (rhs_dim,)), ((), ())), preferred_element_type=F32)


def onehot(values, axis_iota):
    return jnp.where(values == axis_iota, 1.0, 0.0).astype(BF16)


def as_column(row):
    return jnp.broadcast_to(row, (TILE, row.shape[1])).T[:, 0:1]


def gate_parts(gate):
    high = gate.astype(BF16).astype(F32)
    middle = (gate - high).astype(BF16).astype(F32)
    low = gate - high - middle
    lane = lax.broadcasted_iota(jnp.int32, (gate.shape[0], TILE), 1)
    return jnp.where(lane == 0, high, jnp.where(lane == 1, middle, jnp.where(lane == 2, low, 0.0))).astype(BF16)


def flip(me, step):
    out = 0
    for weight in (4, 2, 1):
        mine = (me // weight) % 2
        mask = (step // weight) % 2
        out = out + weight * (mine + mask - 2 * mine * mask)
    return out


def stage_order(turn):
    pair, odd = turn // 2, turn % 2
    middle = ((pair + 1) // 2) % 2
    return middle * (1 + pair + 2 * odd) + (1 - middle) * (6 * (pair // 3) + odd)


def plane_order(turn):
    pair, odd = turn // 2, turn % 2
    opening = 1 - (pair + 1) // 2
    return opening * (6 + odd) + (1 - opening) * (3 + pair - 2 * odd)


def greet_all(n_stage, n_group):
    stage, me = lax.axis_index('stage'), lax.axis_index('expert')
    barrier = pltpu.get_barrier_semaphore()
    for ds in range(n_stage):
        for dk in range(n_group):
            if ds or dk:
                pl.semaphore_signal(barrier, inc=1, device_id=((stage + ds) % n_stage, (me + dk) % n_group), device_id_type=MESH)
    pl.semaphore_wait(barrier, n_stage * n_group - 1)


def swiglu_grads(pre, grad_hid):
    ff = grad_hid.shape[1]
    pre_a, pre_b = pre[:, :ff], pre[:, ff:]
    sig_a = jax.nn.sigmoid(pre_a)
    act_a = pre_a * sig_a
    hidden = (act_a * pre_b).astype(BF16)
    grad_a = (grad_hid * pre_b * sig_a * (1.0 + pre_a * (1.0 - sig_a))).astype(BF16)
    grad_b = (grad_hid * act_a).astype(BF16)
    return hidden, jnp.concatenate([grad_a, grad_b], axis=1)


def dispatch_kernel(n_local, n_rows, x_hbm, dy_hbm, ordx_ref, meta_ref, u1_hbm, u3_hbm, u2_hbm,
                    xs_hbm, dys_hbm, hdd_hbm, pos_ref, bounds_ref, ordz, p0, p1, p2, p3,
                    x_v, dy_v, xp, dyp, xr, dyr, meta_r, xs, dys, hdd, hddk, u13, u2, grads, half,
                    load_sem, xs_send, xs_recv, dy_send, dy_recv, m_send, m_recv, z_send, z_recv, h_send, h_recv, out_sem):
    stage, me = lax.axis_index('stage'), lax.axis_index('expert')
    chip, core = me // 2, me % 2
    n_group, cap = xr.shape[0], xr.shape[1]
    n_tok = x_v.shape[0]
    n_pos = n_rows - TILE
    ff = u2.shape[0]
    loads = [pltpu.make_async_copy(src, dst, load_sem.at[k]) for k, (src, dst) in enumerate((
        (x_hbm, x_v), (dy_hbm, dy_v), (u1_hbm, u13.at[:, pl.ds(0, ff)]), (u3_hbm, u13.at[:, pl.ds(ff, ff)]), (u2_hbm, u2)))]
    for load in loads:
        load.start()
    greet_all(2, n_group)

    def meta_copy(step):
        peer = flip(me, step)
        return pltpu.make_async_remote_copy(src_ref=meta_ref.at[peer], dst_ref=meta_r.at[step], send_sem=m_send.at[step],
                                            recv_sem=m_recv.at[step], device_id=(1 - stage, peer), device_id_type=MESH)

    def x_copy(step):
        return pltpu.make_async_remote_copy(src_ref=xp.at[step], dst_ref=xr.at[step], send_sem=xs_send.at[step],
                                            recv_sem=xs_recv.at[step], device_id=(1 - stage, flip(me, step)), device_id_type=MESH)

    def dy_copy(step):
        return pltpu.make_async_remote_copy(src_ref=dyp.at[step], dst_ref=dyr.at[step], send_sem=dy_send.at[step],
                                            recv_sem=dy_recv.at[step], device_id=(stage, flip(me, step)), device_id_type=MESH)

    def half_copy():
        n = half.shape[0]
        return pltpu.make_async_remote_copy(src_ref=grads.at[pl.ds(pl.multiple_of((1 - core) * n, n), n)], dst_ref=half, send_sem=h_send,
                                            recv_sem=h_recv, device_id=(stage, flip(me, 1)), device_id_type=MESH)

    def order_copy():
        return pltpu.make_async_remote_copy(src_ref=ordx_ref, dst_ref=ordz, send_sem=z_send, recv_sem=z_recv,
                                            device_id=(1 - stage, me), device_id_type=MESH)

    order_copy().start()
    for step in range(n_group):
        meta_copy(step).start()
    loads[0].wait()

    def permuted(order, src):
        return dot(onehot(as_column(order), lax.broadcasted_iota(jnp.int32, (cap, n_tok), 1)), src[...]).astype(BF16)

    def prepare_x(turn):
        step = stage_order(turn)
        xp[step] = permuted(ordx_ref[flip(me, step)], x_v)

    def prepare_dy(turn):
        plane = plane_order(turn)
        dyp[plane] = permuted(ordz[flip(me, plane)], dy_v)

    def place_rows(step, ref, block):
        pos = pos_ref[step]
        n = n_pos // PLACE

        def place_tile(blk, carry):
            rows = pl.ds(pl.multiple_of(blk * n, n), n)
            place = onehot(pos, lax.broadcasted_iota(jnp.int32, (n, cap), 0) + blk * n)
            ref[rows, :] += dot(place, block[...]).astype(BF16)
            return carry

        lax.fori_loop(0, PLACE, place_tile, 0)

    def shared_block(step):
        x_blk, dy_blk = xr[step], dyr[step]
        hidden, grad_ab = swiglu_grads(dot(x_blk, u13[...]), dot(dy_blk, u2[...], 1, 1))
        hddk[:, :ff] = hidden
        hddk[:, ff:3 * ff] = grad_ab
        hddk[:, 3 * ff:] = gate_parts(as_column(meta_r[step, 1:2, :]))
        grads[:, :2 * ff] += dot(x_blk, grad_ab, 0, 0)
        grads[:, 2 * ff:] += dot(dy_blk, hidden, 0, 0)
        place_rows(step, hdd, hddk)

    def merge_step(turn):
        @pl.when(turn < 6)
        def _():
            place_rows(plane_order(turn), dys, dyr.at[plane_order(turn)])

        @pl.when(turn < 2)
        def _():
            @pl.when(turn == 1)
            def _():
                dy_copy(1).wait()
            place_rows(turn, dys, dyr.at[turn])

        def shared_turn(back, carry):
            @pl.when(jnp.where(back == 0, (turn > 2) & (turn < 6), (turn < 2) | (turn > 4)))
            def _():
                shared_block(stage_order(turn - 1 + back))
            return carry

        lax.fori_loop(0, 2, shared_turn, 0)
        place_rows(stage_order(turn), xs, xr.at[stage_order(turn)])

    def positions():
        for step in range(n_group):
            meta_copy(step).wait()
        sub = lax.broadcasted_iota(jnp.int32, (n_local, cap), 0).astype(F32)
        hits = [jnp.where(meta_r[step, 0:1, :] == sub, 1.0, 0.0) for step in range(n_group)]
        counts = [jnp.sum(hit, axis=1, keepdims=True) for hit in hits]
        total = sum(counts[1:], counts[0])
        units = jnp.floor((total + (ALIGN - 1)) * (1.0 / ALIGN))
        lower = jnp.where(lax.broadcasted_iota(jnp.int32, (n_local, n_local), 1) < lax.broadcasted_iota(jnp.int32, (n_local, n_local), 0), 1.0, 0.0)
        first = dot(lower.astype(BF16), jnp.broadcast_to(units, (n_local, TILE)).astype(BF16)) * float(ALIGN)
        bounds_ref[0] = first.astype(jnp.int32)
        bounds_ref[1] = jnp.broadcast_to(total, (n_local, TILE)).astype(jnp.int32)
        earlier = jnp.where(lax.broadcasted_iota(jnp.int32, (cap, cap), 0) < lax.broadcasted_iota(jnp.int32, (cap, cap), 1), 1.0, 0.0).astype(BF16)
        base = first[:, 0:1]
        for step in range(n_group):
            rank = dot(hits[step].astype(BF16), earlier) + base
            pos_ref[step] = jnp.sum(hits[step] * rank, axis=0, keepdims=True).astype(jnp.int32)
            base = base + counts[step]

    def both(index, carry):
        turn = index - AHEAD - 1
        ready = index

        @pl.when(turn >= 0)
        def _():
            x_copy(stage_order(turn)).wait()

            @pl.when(turn + AHEAD < n_group)
            def _():
                x_copy(stage_order(turn + AHEAD)).start()

            @pl.when(turn < 6)
            def _():
                dy_copy(plane_order(turn)).wait()

            @pl.when(turn + AHEAD < 6)
            def _():
                dy_copy(plane_order(turn + AHEAD)).start()
            merge_step(turn)

        @pl.when(ready < n_group)
        def _():
            prepare_x(ready)

            @pl.when(ready < AHEAD)
            def _():
                x_copy(stage_order(ready)).start()

        @pl.when(ready == 0)
        def _():
            loads[1].wait()
            order_copy().wait()

        @pl.when(ready < 6)
        def _():
            prepare_dy(ready)

            @pl.when(ready < AHEAD)
            def _():
                dy_copy(plane_order(ready)).start()

        @pl.when((ready > 0) & (ready < 3))
        def _():
            block = permuted(ordz[flip(me, 2 - ready)], dy_v)

            @pl.when(ready == 1)
            def _():
                dyp[1] = block
                dy_copy(1).start()

            @pl.when(ready == 2)
            def _():
                dyr[0] = block
                for ref in (xs, dys, hdd):
                    ref[...] = jnp.zeros(ref.shape, BF16)
                grads[...] = jnp.zeros(grads.shape, F32)
                positions()
                for load in loads[2:]:
                    load.wait()

        @pl.when(turn == 5)
        def _():
            outs[1].start()
        return carry

    outs = [pltpu.make_async_copy(src, dst, out_sem.at[k]) for k, (src, dst) in enumerate(((xs, xs_hbm), (dys, dys_hbm), (hdd, hdd_hbm)))]
    lax.fori_loop(0, n_group + AHEAD + 1, both, 0)
    half_copy().start()
    outs[0].start()
    outs[2].start()
    half_copy().wait()
    n = p0.shape[0]
    for hop, ref in enumerate((p0, p1, p2, p3)):
        there = flip(me, 2 * hop) // 2
        ref[...] = grads[pl.ds(pl.multiple_of((4 * core + there) * n, n), n), :] + half[pl.ds(pl.multiple_of(there * n, n), n), :]
    for out in outs:
        out.wait()


def dispatch(x_tok, dy_tok, ordx, meta, u1, u3, u2, n_local, n_rows):
    n_group, cap = meta.shape[0], meta.shape[2]
    n_tok, width = x_tok.shape
    ff = u1.shape[1]
    any_spec = pl.BlockSpec(memory_space=pl.ANY)
    vmem_spec = pl.BlockSpec(memory_space=pltpu.VMEM)
    dma = pltpu.SemaphoreType.DMA
    blocks = pltpu.VMEM((n_group, cap, width), BF16)
    part = jax.ShapeDtypeStruct((width // n_group, 3 * ff), F32)
    return pl.pallas_call(
        functools.partial(dispatch_kernel, n_local, n_rows),
        out_shape=(jax.ShapeDtypeStruct((n_rows, width), BF16), jax.ShapeDtypeStruct((n_rows, width), BF16),
                   jax.ShapeDtypeStruct((n_rows, 3 * ff + TILE), BF16), jax.ShapeDtypeStruct((n_group, 1, cap), jnp.int32),
                   jax.ShapeDtypeStruct((2, n_local, TILE), jnp.int32),
                   jax.ShapeDtypeStruct(ordx.shape, jnp.int32), part, part, part, part),
        in_specs=[any_spec, any_spec, vmem_spec, vmem_spec, any_spec, any_spec, any_spec],
        out_specs=(any_spec, any_spec, any_spec) + (vmem_spec,) * 7,
        scratch_shapes=[pltpu.VMEM((n_tok, width), BF16), pltpu.VMEM((n_tok, width), BF16), blocks, blocks, blocks, blocks,
                        pltpu.VMEM(meta.shape, F32), pltpu.VMEM((n_rows, width), BF16), pltpu.VMEM((n_rows, width), BF16),
                        pltpu.VMEM((n_rows, 3 * ff + TILE), BF16), pltpu.VMEM((cap, 3 * ff + TILE), BF16),
                        pltpu.VMEM((width, 2 * ff), BF16), pltpu.VMEM((ff, width), BF16),
                        pltpu.VMEM((width, 3 * ff), F32), pltpu.VMEM((width // 2, 3 * ff), F32),
                        dma((5,)), dma((n_group,)), dma((n_group,)), dma((n_group,)), dma((n_group,)), dma((n_group,)), dma((n_group,)),
                        dma, dma, dma, dma, dma((3,))],
        compiler_params=pltpu.CompilerParams(collective_id=0, has_side_effects=True, vmem_limit_bytes=VMEM_BYTES),
        name='dispatch',
    )(x_tok, dy_tok, ordx, meta, u1, u3, u2)


N_IN = 3
N_CHUNK = 4


def expert_kernel(bounds_ref, xs_hbm, dys_hbm, hdd_hbm, w1, w3, w2, u1_hbm, u3_hbm, u2_hbm,
                  ys_hbm, dxs_hbm, g1, g3, g2,
                  xs, dys, hdd, ys, dxs, u13, u2, w13_v, w2_v, o13, o2, acc13, acc2, sem, rsem, ssem, wsem, osem):
    n_local = w1.shape[0]
    ff = u2.shape[0]
    left, right = pl.ds(0, ff), pl.ds(ff, ff)
    chunk = xs.shape[0] // N_CHUNK
    loads = [pltpu.make_async_copy(src, dst, sem.at[k]) for k, (src, dst) in enumerate((
        (u1_hbm, u13.at[:, left]), (u3_hbm, u13.at[:, right]), (u2_hbm, u2)))]

    def row_loads(part):
        rows = pl.ds(pl.multiple_of(part * chunk, ALIGN), chunk)
        return [pltpu.make_async_copy(src.at[rows], dst.at[rows], rsem.at[part, k])
                for k, (src, dst) in enumerate(((xs_hbm, xs), (dys_hbm, dys), (hdd_hbm, hdd)))]

    def row_stores(part):
        rows = pl.ds(pl.multiple_of(part * chunk, ALIGN), chunk)
        return [pltpu.make_async_copy(src.at[rows], dst.at[rows], ssem.at[part, k]) for k, (src, dst) in enumerate(((ys, ys_hbm), (dxs, dxs_hbm)))]

    def weight_copies(expert):
        slot = lax.rem(expert, N_IN)
        return [pltpu.make_async_copy(w1.at[expert], w13_v.at[slot, :, left], wsem.at[slot, 0]),
                pltpu.make_async_copy(w3.at[expert], w13_v.at[slot, :, right], wsem.at[slot, 1]),
                pltpu.make_async_copy(w2.at[expert], w2_v.at[slot], wsem.at[slot, 2])]

    def grad_copies(expert):
        slot = lax.rem(expert, 2)
        return [pltpu.make_async_copy(o13.at[slot, :, left], g1.at[expert], osem.at[slot, 0]),
                pltpu.make_async_copy(o13.at[slot, :, right], g3.at[expert], osem.at[slot, 1]),
                pltpu.make_async_copy(o2.at[slot], g2.at[expert], osem.at[slot, 2])]

    for copy in row_loads(0) + weight_copies(0) + loads + weight_copies(1):
        copy.start()
    for part in range(1, N_CHUNK):
        for copy in row_loads(part):
            copy.start()
    for copy in weight_copies(2):
        copy.start()
    for ref in (ys, dxs):
        ref[...] = jnp.zeros(ref.shape, BF16)
    for load in loads:
        load.wait()

    def wait_rows(part, carry):
        for copy in row_loads(part):
            copy.wait()
        return carry

    def store_rows(part, carry):
        for copy in row_stores(part):
            copy.start()
        return carry

    def expert_step(expert, carry):
        loaded, stored = carry
        slot, oslot = lax.rem(expert, N_IN), lax.rem(expert, 2)
        for copy in weight_copies(expert):
            copy.wait()

        @pl.when(expert >= 2)
        def _():
            for copy in grad_copies(expert - 2):
                copy.wait()
        first, count = bounds_ref[0, expert, 0], bounds_ref[1, expert, 0]
        need = (first + jnp.maximum((count + TILE - 1) // TILE, 1) * TILE + chunk - 1) // chunk
        lax.fori_loop(loaded, need, wait_rows, 0)

        def rows_pass(begin, n):
            rows = pl.ds(pl.multiple_of(first + begin, ALIGN), n)
            x_blk, parts = xs[rows, :], hdd[rows, 3 * ff:].astype(F32)
            gate = parts[:, 0:1] + parts[:, 1:2] + parts[:, 2:3]
            live = lax.broadcasted_iota(jnp.int32, (n, 1), 0) + begin < count
            grad_out = jnp.where(live, gate * dys[rows, :].astype(F32), 0.0).astype(BF16)
            hidden, grad_ab = swiglu_grads(dot(x_blk, w13_v[slot]), dot(grad_out, w2_v[slot], 1, 1))
            ys[rows, :] = (gate * dot(hidden, w2_v[slot]) + dot(hdd[rows, :ff], u2[...])).astype(BF16)
            dxs[rows, :] = (dot(grad_ab, w13_v[slot], 1, 1) + dot(hdd[rows, ff:3 * ff], u13[...], 1, 1)).astype(BF16)
            return dot(x_blk, grad_ab, 0, 0), dot(hidden, grad_out, 0, 0)

        for n in (1, 2, 3):
            @pl.when((count > (n - 1) * TILE if n > 1 else count >= 0) & (count <= n * TILE))
            def _():
                grad13, grad2 = rows_pass(0, n * TILE)
                o13[oslot] = grad13.astype(BF16)
                o2[oslot] = grad2.astype(BF16)

        @pl.when(count > 3 * TILE)
        def _():
            acc13[...] = jnp.zeros(acc13.shape, F32)
            acc2[...] = jnp.zeros(acc2.shape, F32)

            def tile_step(tile, inner):
                grad13, grad2 = rows_pass(tile * TILE, TILE)
                acc13[...] += grad13
                acc2[...] += grad2
                return inner

            lax.fori_loop(0, (count + TILE - 1) // TILE, tile_step, 0)
            o13[oslot] = acc13[...].astype(BF16)
            o2[oslot] = acc2[...].astype(BF16)

        for copy in grad_copies(expert):
            copy.start()

        @pl.when(expert + N_IN < n_local)
        def _():
            for copy in weight_copies(expert + N_IN):
                copy.start()
        final = (first + (count + ALIGN - 1) // ALIGN * ALIGN) // chunk
        lax.fori_loop(stored, final, store_rows, 0)
        return jnp.maximum(loaded, need), jnp.maximum(stored, final)

    loaded, stored = lax.fori_loop(0, n_local, expert_step, (0, 0))
    lax.fori_loop(loaded, N_CHUNK, wait_rows, 0)
    lax.fori_loop(stored, N_CHUNK, store_rows, 0)
    for copy in grad_copies(n_local - 2) + grad_copies(n_local - 1):
        copy.wait()
    for part in range(N_CHUNK):
        for copy in row_stores(part):
            copy.wait()


def experts(bounds, xs, dys, hdd, w1, w3, w2, u1, u3, u2):
    n_rows, width = xs.shape
    ff = w1.shape[2]
    any_spec = pl.BlockSpec(memory_space=pl.ANY)
    smem_spec = pl.BlockSpec(memory_space=pltpu.SMEM)
    rows = pltpu.VMEM((n_rows, width), BF16)
    return pl.pallas_call(
        expert_kernel,
        in_specs=[smem_spec, any_spec, any_spec, any_spec] + [any_spec] * 6,
        out_specs=(any_spec,) * 5,
        out_shape=(jax.ShapeDtypeStruct((n_rows, width), BF16), jax.ShapeDtypeStruct((n_rows, width), BF16),
                   jax.ShapeDtypeStruct(w1.shape, BF16), jax.ShapeDtypeStruct(w3.shape, BF16), jax.ShapeDtypeStruct(w2.shape, BF16)),
        scratch_shapes=[rows, rows, pltpu.VMEM(hdd.shape, BF16), rows, rows,
                        pltpu.VMEM((width, 2 * ff), BF16), pltpu.VMEM((ff, width), BF16),
                        pltpu.VMEM((N_IN, width, 2 * ff), BF16), pltpu.VMEM((N_IN, ff, width), BF16),
                        pltpu.VMEM((2, width, 2 * ff), BF16), pltpu.VMEM((2, ff, width), BF16),
                        pltpu.VMEM((width, 2 * ff), F32), pltpu.VMEM((ff, width), F32),
                        pltpu.SemaphoreType.DMA((3,)), pltpu.SemaphoreType.DMA((N_CHUNK, 3)), pltpu.SemaphoreType.DMA((N_CHUNK, 2)),
                        pltpu.SemaphoreType.DMA((N_IN, 3)), pltpu.SemaphoreType.DMA((2, 3))],
        compiler_params=pltpu.CompilerParams(vmem_limit_bytes=VMEM_BYTES),
        cost_estimate=pl.CostEstimate(flops=40_000_000_000, bytes_accessed=100_000_000, transcendentals=0),
        name='experts',
    )(bounds, xs, dys, hdd, w1, w3, w2, u1, u3, u2)


def return_kernel(ys_hbm, dxs_hbm, pos_ref, ordx_ref, ordy_ref, p0, r1, r2, r3, y_ref, dx_ref, f1, f3, f2,
                  ys, dxs, yp, dxp, yr, dxr, own, own2, all13, all2,
                  load_sem, y_send, y_recv, dx_send, dx_recv, all_send, all_recv, pair_send, pair_recv):
    stage, me = lax.axis_index('stage'), lax.axis_index('expert')
    n_group, cap = yr.shape[0], yr.shape[1]
    n_tok = y_ref.shape[0]
    n_pos = ys.shape[0]
    n_chip = n_group // 2
    chip, core = me // 2, me % 2
    ff = f1.shape[1]
    n_part = own.shape[0]
    load_y = pltpu.make_async_copy(ys_hbm.at[pl.ds(0, n_pos)], ys, load_sem.at[0])
    load_dx = pltpu.make_async_copy(dxs_hbm.at[pl.ds(0, n_pos)], dxs, load_sem.at[1])
    load_dx.start()
    load_y.start()
    greet_all(2, n_group)

    def y_copy(step):
        return pltpu.make_async_remote_copy(src_ref=yp.at[step], dst_ref=yr.at[step], send_sem=y_send.at[step],
                                            recv_sem=y_recv.at[step], device_id=(stage, flip(me, step)), device_id_type=MESH)

    def dx_copy(step):
        return pltpu.make_async_remote_copy(src_ref=dxp.at[step], dst_ref=dxr.at[step], send_sem=dx_send.at[step],
                                            recv_sem=dx_recv.at[step], device_id=(1 - stage, flip(me, step)), device_id_type=MESH)

    def all_copies(hop, landing):
        there = flip(me, 2 * hop)
        slot = n_chip * core + (there // 2 if landing else chip)
        return [pltpu.make_async_remote_copy(src_ref=src, dst_ref=dst.at[slot], send_sem=all_send.at[2 * hop - 2 + k],
                                             recv_sem=all_recv.at[2 * hop - 2 + k], device_id=(stage, there), device_id_type=MESH)
                for k, (src, dst) in enumerate(((own, all13), (own2, all2)))]

    def pair_copies(landing):
        rows = pl.ds(((1 - core) if landing else core) * n_chip, n_chip)
        return [pltpu.make_async_remote_copy(src_ref=ref.at[rows], dst_ref=ref.at[rows], send_sem=pair_send.at[k],
                                             recv_sem=pair_recv.at[k], device_id=(stage, flip(me, 1)), device_id_type=MESH)
                for k, ref in enumerate((all13, all2))]

    part = p0[...] + r1[...] + r2[...] + r3[...]
    own[...] = part[:, :2 * ff].astype(BF16)
    own2[...] = part[:, 2 * ff:].T.astype(BF16)
    all13[n_chip * core + chip] = part[:, :2 * ff].astype(BF16)
    all2[n_chip * core + chip] = part[:, 2 * ff:].T.astype(BF16)
    load_dx.wait()

    def picked(step, src):
        return dot(onehot(as_column(pos_ref[step]), lax.broadcasted_iota(jnp.int32, (cap, n_pos), 1)), src[...]).astype(BF16)

    def home_rows(order, ref, block):
        n = n_tok // PLACE

        def home_tile(blk, carry):
            rows = pl.ds(pl.multiple_of(blk * n, n), n)
            tok = lax.broadcasted_iota(jnp.int32, (n, cap), 0) + blk * n
            ref[rows, :] += dot(onehot(order, tok), block[...]).astype(BF16)
            return carry

        lax.fori_loop(0, PLACE, home_tile, 0)

    def both(index, carry):
        turn = index - AHEAD - 1
        ready = index

        @pl.when(turn >= 0)
        def _():
            dx_copy(stage_order(turn)).wait()

            @pl.when(turn + AHEAD < n_group)
            def _():
                dx_copy(stage_order(turn + AHEAD)).start()

            @pl.when(turn < 6)
            def _():
                y_copy(plane_order(turn)).wait()

            @pl.when(turn + AHEAD < 6)
            def _():
                y_copy(plane_order(turn + AHEAD)).start()

        @pl.when(ready < n_group)
        def _():
            dxp[stage_order(ready)] = picked(stage_order(ready), dxs)

            @pl.when(ready < AHEAD)
            def _():
                dx_copy(stage_order(ready)).start()

        @pl.when(ready == 0)
        def _():
            load_y.wait()

        @pl.when(ready < 6)
        def _():
            yp[plane_order(ready)] = picked(plane_order(ready), ys)

            @pl.when(ready < AHEAD)
            def _():
                y_copy(plane_order(ready)).start()

        @pl.when((ready > 0) & (ready < 3))
        def _():
            block = picked(2 - ready, ys)

            @pl.when(ready == 1)
            def _():
                yp[1] = block
                y_copy(1).start()

            @pl.when(ready == 2)
            def _():
                yr[0] = block
                y_ref[...] = jnp.zeros(y_ref.shape, BF16)
                dx_ref[...] = jnp.zeros(dx_ref.shape, BF16)
                for hop in (1, 2, 3):
                    for copy in all_copies(hop, False):
                        copy.start()

        @pl.when(turn == 6)
        def _():
            for hop in (1, 2, 3):
                for copy in all_copies(hop, False):
                    copy.wait_send()
                for copy in all_copies(hop, True):
                    copy.wait_recv()
            for copy in pair_copies(False):
                copy.start()

        @pl.when(turn == 7)
        def _():
            for copy in pair_copies(False):
                copy.wait_send()
            for copy in pair_copies(True):
                copy.wait_recv()
            for k in range(n_group):
                rows = pl.ds(k * n_part, n_part)
                f1[rows, :] = all13[k, :, :ff]
                f3[rows, :] = all13[k, :, ff:]
                f2[:, rows] = all2[k]

        @pl.when((turn == 1) | (turn == 2))
        def _():
            step = 2 - turn

            @pl.when(step == 1)
            def _():
                y_copy(1).wait()
            home_rows(ordy_ref[flip(me, step)], y_ref, yr.at[step])

        @pl.when(turn >= 0)
        def _():
            @pl.when(turn < 6)
            def _():
                home_rows(ordy_ref[flip(me, plane_order(turn))], y_ref, yr.at[plane_order(turn)])
            home_rows(ordx_ref[flip(me, stage_order(turn))], dx_ref, dxr.at[stage_order(turn)])
        return carry

    lax.fori_loop(0, n_group + AHEAD + 1, both, 0)


def give_back(ys, dxs, pos, ordx, ordy, p0, r1, r2, r3, n_tok):
    n_group, cap = ordx.shape[0], ordx.shape[2]
    n_rows, width = ys.shape
    n_pos = n_rows - TILE
    n_part, ff = p0.shape[0], p0.shape[1] // 3
    any_spec = pl.BlockSpec(memory_space=pl.ANY)
    vmem_spec = pl.BlockSpec(memory_space=pltpu.VMEM)
    dma = pltpu.SemaphoreType.DMA
    blocks = pltpu.VMEM((n_group, cap, width), BF16)
    in_shape = jax.ShapeDtypeStruct((width, ff), BF16)
    return pl.pallas_call(
        return_kernel,
        out_shape=(jax.ShapeDtypeStruct((n_tok, width), BF16), jax.ShapeDtypeStruct((n_tok, width), BF16),
                   in_shape, in_shape, jax.ShapeDtypeStruct((ff, width), BF16)),
        in_specs=[any_spec, any_spec] + [vmem_spec] * 7,
        out_specs=(vmem_spec,) * 5,
        scratch_shapes=[pltpu.VMEM((n_pos, width), BF16), pltpu.VMEM((n_pos, width), BF16), blocks, blocks, blocks, blocks,
                        pltpu.VMEM((n_part, 2 * ff), BF16), pltpu.VMEM((ff, n_part), BF16),
                        pltpu.VMEM((n_group, n_part, 2 * ff), BF16), pltpu.VMEM((n_group, ff, n_part), BF16),
                        dma((2,)), dma((n_group,)), dma((n_group,)), dma((n_group,)), dma((n_group,)),
                        dma((6,)), dma((6,)), dma((2,)), dma((2,))],
        compiler_params=pltpu.CompilerParams(collective_id=1, has_side_effects=True, vmem_limit_bytes=VMEM_BYTES),
        name='give_back',
    )(ys, dxs, pos, ordx, ordy, p0, r1, r2, r3)


def solution(mesh):
    n_group = mesh.shape['expert']
    tok_spec = P('stage', 'expert', None)
    w_spec = P('stage', 'expert', None, None)
    sh_spec = P('stage', None, None)

    def device_fn(x_act, route_idx, route_gate, w_in1, w_in3, w_out, ws_in1, ws_in3, ws_out, dy_out):
        n_tok = x_act.shape[1]
        n_local = w_in1.shape[1]
        cap = n_tok // n_group
        n_rows = n_tok + n_local * ALIGN + TILE
        idx = route_idx[0].reshape(n_tok)
        tok_ids = jnp.arange(n_tok, dtype=jnp.int32)
        sorted_idx, order, sorted_gate = lax.sort((idx, tok_ids, route_gate[0].reshape(n_tok)), num_keys=1)
        order = order.reshape(n_group, 1, cap)
        lid = (sorted_idx % n_local).astype(F32).reshape(n_group, 1, cap)
        meta = jnp.concatenate([lid, sorted_gate.reshape(n_group, 1, cap), jnp.zeros((n_group, 6, cap), F32)], axis=1)
        xs, dys, hdd, pos, bounds, order_back, p0, p1, p2, p3 = dispatch(
            x_act[0], dy_out[0], order, meta, ws_in1[0], ws_in3[0], ws_out[0], n_local, n_rows)
        recv = [lax.ppermute(part, 'expert', [(k, k ^ (2 * hop)) for k in range(n_group)]) for hop, part in ((1, p1), (2, p2), (3, p3))]
        ys, dxs, g1, g3, g2 = experts(bounds, xs, dys, hdd,
                                      w_in1[0], w_in3[0], w_out[0], ws_in1[0], ws_in3[0], ws_out[0])
        y_tok, dx_tok, f1, f3, f2 = give_back(ys, dxs, pos, order, order_back, p0, *recv, n_tok)
        return (y_tok[None], dx_tok[None], g1[None], g3[None], g2[None], f1[None], f3[None], f2[None])

    return jax.shard_map(device_fn, mesh=mesh,
                         in_specs=(tok_spec, tok_spec, tok_spec, w_spec, w_spec, w_spec, sh_spec, sh_spec, sh_spec, tok_spec),
                         out_specs=(tok_spec, tok_spec, w_spec, w_spec, w_spec, sh_spec, sh_spec, sh_spec),
                         check_vma=False)
```
